32 devices in a mesh: vp: 32 (over z, y, x, core).
Axes of the slice: x: 2, y: 2, z: 4, core: 2. Of those that a mesh axis runs over, the one named last changes fastest.
Arguments:
- residual: bfloat16 [8192, 4096], replicated
- labels: int32 [8192], replicated
- loss_mask: float32 [8192], replicated
- norm_gain: float32 [4096], replicated
- embed_table: bfloat16 [49408, 4096], P('vp')
Outputs:
- output 1: float32 [], replicated
- output 2: float32 [8192, 4096], P('vp')
- output 3: float32 [49408, 4096], P('vp')
- output 4: float32 [4096], replicated
All inputs are finite; a program needn't handle non-finite values.
Results may differ from the reference program's by a relative error of at most 0.001.
Values sent between devices are 32-bit elements.
A program may use at most 1 GiB of HBM per device.

```python
import jax
import jax.numpy as jnp
from jax import lax

TOKENS = 8192
DIM = 4096
VOCAB_REAL = 49155
VOCAB_PAD = 49408

LOGIT_SCALE = 6.0
NORM_EPS = 1e-6


def draw_labels(label_key):
    k_pick, k_wide, k_low = jax.random.split(label_key, 3)
    pick_wide = jax.random.randint(k_pick, (TOKENS,), 0, 2)
    wide_ids = jax.random.randint(k_wide, (TOKENS,), 0, VOCAB_REAL)
    low_ids = jax.random.randint(k_low, (TOKENS,), 0, VOCAB_REAL // 16)
    label_ids = jnp.where(pick_wide == 0, wide_ids, low_ids).astype(jnp.int32)
    return label_ids.at[0].set(0).at[1].set(VOCAB_REAL - 1)


def draw_mask(mask_key):
    keep_draw = jax.random.randint(mask_key, (TOKENS,), 0, 5)
    mask_vals = (keep_draw > 0).astype(jnp.float32)
    return mask_vals.at[0].set(1.0)


def setup_inputs(seed: int = 0) -> dict:
    base_key = jax.random.key(seed)
    k_table, k_noise, k_peak, k_gain, k_label, k_mask = jax.random.split(base_key, 6)
    emb_std = LOGIT_SCALE * DIM ** -0.5
    table_f32 = jax.random.normal(k_table, (VOCAB_PAD, DIM), jnp.float32) * emb_std
    peak_ids = jax.random.randint(k_peak, (TOKENS, 4), 0, VOCAB_REAL)
    peak_sum = jnp.zeros((TOKENS, DIM), jnp.float32)
    for peak in range(4):
        peak_sum = peak_sum + table_f32[peak_ids[:, peak]] / emb_std
    peak_weight = 14.0 * DIM ** -0.5
    noise = jax.random.normal(k_noise, (TOKENS, DIM), jnp.float32)
    residual = (noise + peak_weight * peak_sum).astype(jnp.bfloat16)
    norm_gain = 1.0 + 0.3 * jax.random.normal(k_gain, (DIM,), jnp.float32)
    return {
        'residual': residual,
        'labels': draw_labels(k_label),
        'loss_mask': draw_mask(k_mask),
        'norm_gain': norm_gain,
        'embed_table': table_f32.astype(jnp.bfloat16),
    }


def reference(residual, labels, loss_mask, norm_gain, embed_table):
    x_f32 = residual.astype(jnp.float32)
    inv_rms = lax.rsqrt(jnp.mean(x_f32 * x_f32, axis=-1, keepdims=True) + NORM_EPS)
    x_hat = x_f32 * inv_rms
    hidden = (x_hat * norm_gain).astype(jnp.bfloat16)
    mask_total = jnp.sum(loss_mask)
    tok_weight = loss_mask / mask_total
    col_ids = jnp.arange(VOCAB_PAD)[None, :]
    row_block = min(TOKENS, 256)
    n_blocks = TOKENS // row_block

    def block_step(grad_table, block_in):
        h_blk, lab_blk, w_blk = block_in
        logits = jnp.dot(h_blk, embed_table.T, preferred_element_type=jnp.float32) / LOGIT_SCALE
        logits = jnp.where(col_ids < VOCAB_REAL, logits, -jnp.inf)
        row_max = jnp.max(logits, axis=-1, keepdims=True)
        shifted = jnp.exp(logits - row_max)
        sum_exp = jnp.sum(shifted, axis=-1, keepdims=True)
        is_label = col_ids == lab_blk[:, None]
        target = jnp.sum(jnp.where(is_label, logits, 0.0), axis=-1)
        tok_loss = row_max[:, 0] + jnp.log(sum_exp[:, 0]) - target
        row_prob = shifted / sum_exp
        d_logits = (jnp.where(is_label, row_prob - 1.0, row_prob) * w_blk[:, None]).astype(jnp.bfloat16)
        d_hidden = jnp.dot(d_logits, embed_table, preferred_element_type=jnp.float32) / LOGIT_SCALE
        grad_table = grad_table + jnp.dot(d_logits.T, h_blk, preferred_element_type=jnp.float32) / LOGIT_SCALE
        return grad_table, (tok_loss, d_hidden)

    blocks = (hidden.reshape(n_blocks, row_block, DIM), labels.reshape(n_blocks, row_block), tok_weight.reshape(n_blocks, row_block))
    d_embed, (tok_loss, d_hidden) = lax.scan(block_step, jnp.zeros((VOCAB_PAD, DIM), jnp.float32), blocks)
    tok_loss = tok_loss.reshape(TOKENS)
    d_hidden = d_hidden.reshape(TOKENS, DIM)
    mean_loss = jnp.sum(loss_mask * tok_loss) / mask_total
    d_gain = jnp.sum(d_hidden * x_hat, axis=0)
    d_xhat = d_hidden * norm_gain
    d_residual = inv_rms * (d_xhat - x_hat * jnp.mean(d_xhat * x_hat, axis=-1, keepdims=True))
    return (mean_loss, d_residual, d_embed, d_gain)
```

```python
import functools

import jax
import jax.numpy as jnp
from jax import lax
from jax.experimental import pallas as pl
from jax.experimental.pallas import tpu as pltpu
from jax.sharding import PartitionSpec as P

VOCAB_REAL = 49155
LOGIT_SCALE = 6.0
NORM_EPS = 1e-6
MESH = pl.DeviceIdType.MESH

GROUP = 8
ROWS = 32 * GROUP
COL_A, COL_B, COL_C = 896, 1792, 1408
DEPTH = 6


def step_kernel(
    n_chunks, res, lab, wgt, gain, tab,
    dx_out, de_out, dg_out, loss_out,
    ev, h, zt, dzt, dz, acc, op, r0,
    r1a, r1b, r1c, r2c, zra, zla, zrb, zlb, zrc, zlc,
    fsa, fka, r3a, fsb, fkb, r3b,
    st, tacc, ssq, dhf, xr, dxb, dgacc, dg1, dg2,
    sem_in, sem_out, sem_p, cred, nbr, sem_st, sem_g1, sem_g2,
    sem_a, sem_b, sem_c,
):
    vocab, width = ev.shape
    edges = list(range(0, max(vocab - 511, 1), 512)) + [vocab]
    blocks = [(a, b - a) for a, b in zip(edges, edges[1:])]
    me = lax.axis_index("vp")
    c, x, y, z = me % 2, (me // 2) % 2, (me // 4) % 2, me // 8

    def dev(zz, yy, xx, cc):
        return (((zz * 2 + yy) * 2 + xx) * 2 + cc,)

    def send(src, dst, ssem, rsem, to):
        return pltpu.make_async_remote_copy(src, dst, ssem, rsem, device_id=to, device_id_type=MESH)

    nbr_x, nbr_y = dev(z, y, 1 - x, c), dev(z, 1 - y, x, c)
    nbr_r, nbr_l = dev(z + 1, y, x, c), dev(z - 1, y, x, c)
    partner = dev(z, y, x, 1 - c)

    def load_x(n, half):
        return pltpu.make_async_copy(res.at[:, half, n], h.at[n % 2, pl.ds(16 * half, 16)], sem_in.at[half])

    def load_own(n):
        return pltpu.make_async_copy(res.at[me // 2, me % 2, n], xr.at[n % 2], sem_in.at[2 + n % 2])

    def store_dx(n):
        return pltpu.make_async_copy(dxb.at[n % 2], dx_out.at[n], sem_out.at[n % 2])

    def norm(n):
        slot = n % 2
        g = gain[...]

        def squares(i, _):
            xt = h[slot, i].astype(jnp.float32)
            sq = xt * xt
            ssq[i] = sum(sq[:, j : j + 128] for j in range(0, width, 128))
            return 0

        def scale(i, _):
            inv = ssq[i][:, 0:1]
            xt = h[slot, i].astype(jnp.float32)
            h[slot, i] = ((xt * inv) * g).astype(jnp.bfloat16)
            return 0

        lax.fori_loop(0, 32, squares, 0, unroll=4)
        mean = jnp.sum(ssq[...], axis=-1, keepdims=True) * (1.0 / width)
        ssq[...] = jnp.broadcast_to(lax.rsqrt(mean + NORM_EPS), ssq.shape)
        lax.fori_loop(0, 32, scale, 0, unroll=4)

    def logits(n):
        top = jnp.full((1, ROWS), -jnp.inf, jnp.float32)
        hn = h[n % 2].reshape(ROWS, width)
        for a, m in blocks:
            t = lax.dot_general(ev[a : a + m, :], hn, (((1,), (1,)), ((), ())), preferred_element_type=jnp.float32)
            t = t / LOGIT_SCALE
            ids = me * vocab + a + lax.broadcasted_iota(jnp.int32, (m, ROWS), 0)
            t = jnp.where(ids < VOCAB_REAL, t, -jnp.inf)
            zt[a : a + m, :] = t
            top = jnp.maximum(top, jnp.max(t, axis=0, keepdims=True))
        return top

    full_tiles = vocab // 128
    tail = vocab - full_tiles * 128

    def local_lse(n, top):
        lb = lab[pl.ds(n, 1), :] - me * vocab

        def part(a, m, s, t):
            v = zt[pl.ds(a, m), :]
            ids = a + lax.broadcasted_iota(jnp.int32, (m, ROWS), 0)
            e = jnp.exp(v - top).reshape(m // 8, 8, ROWS)
            hit = jnp.where(ids == lb, v, 0.0).reshape(m // 8, 8, ROWS)
            return s + jnp.sum(e, axis=0), t + jnp.sum(hit, axis=0)

        zero = jnp.zeros((8, ROWS), jnp.float32)
        s, t = lax.fori_loop(0, full_tiles, lambda i, v: part(pl.multiple_of(i * 128, 128), 128, *v), (zero, zero))
        s, t = part(full_tiles * 128, tail, s, t)
        tacc[1:2, :] += wgt[pl.ds(n, 1), :] * jnp.sum(t, axis=0, keepdims=True)
        return top + jnp.log(jnp.sum(s, axis=0, keepdims=True))

    def merge(ref, slot, count):
        rows = [ref[slot, q] for q in range(count)]
        top = functools.reduce(jnp.maximum, rows)
        return top + jnp.log(sum(jnp.exp(r - top) for r in rows))

    def grad_logits(k, lse):
        lb = lab[pl.ds(k, 1), :] - me * vocab
        w = wgt[pl.ds(k, 1), :]
        for a, m in [(i * 128, 128) for i in range(full_tiles)] + [(full_tiles * 128, tail)]:
            ids = a + lax.broadcasted_iota(jnp.int32, (m, ROWS), 0)
            p = jnp.exp(zt[a : a + m, :] - lse)
            d = (jnp.where(ids == lb, p - 1.0, p) * w).astype(jnp.bfloat16)
            dzt[a : a + m, :] = d
            dz[:, a : a + m] = d.T

    def embed_grad(k):
        tile = width // 4
        for a, m in blocks:
            for j in range(4):
                cols = pl.ds(j * tile, tile)
                acc[a : a + m, cols] += jnp.dot(dzt[a : a + m, :], h[k % 2, :, :, cols].reshape(ROWS, tile), preferred_element_type=jnp.float32)

    def send_p(half):
        cols = pl.ds(half * (width // 2), width // 2)
        return send(op.at[2, :, :, :, :, cols], r0.at[:, :, :, :, cols], sem_p.at[0, half], sem_p.at[1, half], partner)

    def hidden_grad(k):
        own = k % 2
        eq0 = 1 - c
        where = (eq0 * own + (1 - eq0) * 2, c * own + (1 - c) * 2)
        for half in range(2):
            cols = pl.ds(half * (width // 2), width // 2)
            r = jnp.dot(dz[...], ev[:, cols], preferred_element_type=jnp.float32)
            for q in range(2):
                op[where[q], :, :, :, :, cols] = r[q * 128 : (q + 1) * 128].reshape(4, 2, 2, 8, width // 2)
            if half == 0:
                @pl.when(k >= 1)
                def _():
                    pl.semaphore_wait(cred, 1)
            send_p(half).start()

    def add_partner(k):
        for half in range(2):
            send_p(half).wait()

        def body(i, _):
            op[k % 2, i] += r0[i]
            return 0

        lax.fori_loop(0, 4, body, 0)

        @pl.when(k < n_chunks - 1)
        def _():
            pl.semaphore_signal(cred, 1, device_id=partner, device_id_type=MESH)

    def swap8(buf, slot, sem):
        out = []
        for q in range(1, 8):
            qy, qx, qc = q // 4, (q // 2) % 2, q % 2
            to = dev(z, y + qy * (1 - 2 * y), x + qx * (1 - 2 * x), c + qc * (1 - 2 * c))
            out.append(send(buf.at[slot, 0], buf.at[slot, q], sem.at[0, slot, q], sem.at[1, slot, q], to))
        return out

    def swap32(buf, slot, sem):
        out = []
        for q in range(1, 32):
            qz, qy, qx, qc = q // 8, (q // 4) % 2, (q // 2) % 2, q % 2
            to = dev((z + qz) % 4, y + qy * (1 - 2 * y), x + qx * (1 - 2 * x), c + qc * (1 - 2 * c))
            there = ((4 - qz) % 4) * 8 + q % 8
            out.append(send(buf.at[slot, 0], buf.at[slot, there], sem.at[0, slot, q], sem.at[1, slot, there], to))
        return out

    def swap4(buf, slot, sem):
        out = []
        for q in range(1, 4):
            out.append(send(buf.at[slot, 0], buf.at[slot, 4 - q], sem.at[0, slot, q], sem.at[1, slot, 4 - q], dev((z + q) % 4, y, x, c)))
        return out

    def start(copies):
        for cp in copies:
            cp.start()

    def wait(copies):
        for cp in copies:
            cp.wait_send()
        for cp in copies:
            cp.wait_recv()

    def z_copies(zr, zl, s1, sl, t, zslot, sem, par):
        sl_z = zslot[t]
        sl_p = zslot[t - 1] if t else 0
        right = {
            "send": (z <= min(t, 2)),
            "recv": (z >= 1) & (z <= t + 1),
            "first": send(s1.at[sl, 3 - t], zr.at[t, sl_z], sem.at[0, 0, t, par], sem.at[1, 0, t, par], nbr_r),
        }
        left = {
            "send": (z >= 3 - t) & (z >= 1),
            "recv": (z <= 2) & (z >= 2 - t),
            "first": send(s1.at[sl, t], zl.at[t, sl_z], sem.at[0, 1, t, par], sem.at[1, 1, t, par], nbr_l),
        }
        if t:
            right["next"] = send(zr.at[t - 1, sl_p], zr.at[t, sl_z], sem.at[0, 0, t, par], sem.at[1, 0, t, par], nbr_r)
            left["next"] = send(zl.at[t - 1, sl_p], zl.at[t, sl_z], sem.at[0, 1, t, par], sem.at[1, 1, t, par], nbr_l)
        return right, left

    def z_wait(right, left):
        for way in (right, left):
            @pl.when(way["send"])
            def _(way=way):
                way["first"].wait_send()

            @pl.when(way["recv"])
            def _(way=way):
                way["first"].wait_recv()

    def z_start(right, left, zr, zl, s1, sl, t, zslot):
        sl_p = zslot[t - 1] if t else 0

        @pl.when(z == 0)
        def _():
            right["first"].start()

        @pl.when(z == 3)
        def _():
            left["first"].start()

        if t:
            @pl.when((z >= 1) & right["send"])
            def _():
                zr[t - 1, sl_p] += s1[sl, 3 - t + z]
                right["next"].start()

            @pl.when((z <= 2) & left["send"])
            def _():
                zl[t - 1, sl_p] += s1[sl, t - (3 - z)]
                left["next"].start()

    def in_range(k):
        return (k >= 0) & (k < n_chunks)

    def serve_two(s, axis, col, size, r1, zr, zl, fs, fk, r3, sem1, semz, sem3):
        cols = pl.ds(col, size)
        first_nbr, last_nbr = (nbr_x, nbr_y) if axis == "x" else (nbr_y, nbr_x)
        q = y if axis == "x" else x

        def zs(k):
            return (k % 3, k % 3, k % 3)

        def copy1(k):
            src = op.at[k % 2, :, :, 1 - x, :, cols] if axis == "x" else op.at[k % 2, :, 1 - y, :, :, cols]
            return send(src, r1.at[k % 5], sem1.at[0, k % 2], sem1.at[1, k % 2], first_nbr)

        def copy3(k):
            return send(fs, r3.at[k % 2], sem3.at[0, k % 2], sem3.at[1, k % 2], last_nbr)

        def zc(k, t):
            return z_copies(zr, zl, r1, k % 5, t, zs(k), semz, k % 2)

        k = s - 6

        @pl.when(in_range(k))
        def _():
            copy3(k).wait()
            dhf[:, cols] = fk[...] + r3[k % 2]

        k5 = s - 5

        @pl.when(in_range(k5))
        def _():
            z_wait(*zc(k5, 2))
            sl = k5 % 5
            fs[...] = r1[sl, z, 1 - q]
            fk[...] = r1[sl, z, q]

            @pl.when(z >= 1)
            def _():
                fs[...] += zr[2, k5 % 3, 1 - q]
                fk[...] += zr[2, k5 % 3, q]

            @pl.when(z <= 2)
            def _():
                fs[...] += zl[2, k5 % 3, 1 - q]
                fk[...] += zl[2, k5 % 3, q]

            copy3(k5).start()

        for t, back in ((2, 4), (1, 3)):
            kt = s - back

            @pl.when(in_range(kt))
            def _(kt=kt, t=t):
                z_wait(*zc(kt, t - 1))
                z_start(*zc(kt, t), zr, zl, r1, kt % 5, t, zs(kt))

        k2 = s - 2

        @pl.when(in_range(k2))
        def _():
            copy1(k2).wait()
            for b in range(4):
                kept = op[k2 % 2, b, :, x, :, cols] if axis == "x" else op[k2 % 2, b, y, :, :, cols]
                r1[k2 % 5, b] += kept
            z_start(*zc(k2, 0), zr, zl, r1, k2 % 5, 0, zs(k2))

        k1 = s - 1

        @pl.when(in_range(k1))
        def _():
            copy1(k1).start()

    def serve_c(s):
        cols = pl.ds(COL_A + COL_B, COL_C)

        def zs(k):
            return (k % 3, k % 3, k % 3)

        def copy1(k):
            return send(op.at[k % 2, :, :, 1 - x, :, cols], r1c.at[k % 3], sem_c["1"].at[0, k % 2], sem_c["1"].at[1, k % 2], nbr_x)

        def copy2(k):
            return send(r1c.at[k % 3, :, 1 - y], r2c.at[k % 5], sem_c["2"].at[0, k % 2], sem_c["2"].at[1, k % 2], nbr_y)

        def zc(k, t):
            return z_copies(zrc, zlc, r2c, k % 5, t, zs(k), sem_c["z"], k % 2)

        k = s - 6

        @pl.when(in_range(k))
        def _():
            z_wait(*zc(k, 2))
            dhf[:, cols] = r2c[k % 5, z]

            @pl.when(z >= 1)
            def _():
                dhf[:, cols] += zrc[2, k % 3]

            @pl.when(z <= 2)
            def _():
                dhf[:, cols] += zlc[2, k % 3]

        for t, back in ((2, 5), (1, 4)):
            kt = s - back

            @pl.when(in_range(kt))
            def _(kt=kt, t=t):
                z_wait(*zc(kt, t - 1))
                z_start(*zc(kt, t), zrc, zlc, r2c, kt % 5, t, zs(kt))

        k3 = s - 3

        @pl.when(in_range(k3))
        def _():
            copy2(k3).wait()
            for b in range(4):
                r2c[k3 % 5, b] += r1c[k3 % 3, b, y]
            z_start(*zc(k3, 0), zrc, zlc, r2c, k3 % 5, 0, zs(k3))

        k2 = s - 2

        @pl.when(in_range(k2))
        def _():
            copy1(k2).wait()
            for b in range(4):
                r1c[k2 % 3, b] += op[k2 % 2, b, :, x, :, cols]
            copy2(k2).start()

        k1 = s - 1

        @pl.when(in_range(k1))
        def _():
            copy1(k1).start()

    def finish(k):
        load_own(k).wait()

        @pl.when(k >= 2)
        def _():
            store_dx(k - 2).wait()

        xo = xr[k % 2].astype(jnp.float32)
        inv = lax.rsqrt(jnp.mean(xo * xo, axis=-1, keepdims=True) + NORM_EPS)
        xh = xo * inv
        dh = dhf[...] / LOGIT_SCALE
        dgacc[...] += dh * xh
        u = dh * gain[...]
        dxb[k % 2] = inv * (u - xh * jnp.mean(u * xh, axis=-1, keepdims=True))
        store_dx(k).start()

    def tell_neighbours():
        pl.semaphore_signal(nbr.at[0], 1, device_id=nbr_x, device_id_type=MESH)
        pl.semaphore_signal(nbr.at[1], 1, device_id=nbr_y, device_id_type=MESH)

        @pl.when(z <= 2)
        def _():
            pl.semaphore_signal(nbr.at[2], 1, device_id=nbr_r, device_id_type=MESH)

        @pl.when(z >= 1)
        def _():
            pl.semaphore_signal(nbr.at[3], 1, device_id=nbr_l, device_id_type=MESH)

    def hear_neighbours():
        pl.semaphore_wait(nbr.at[0], 1)
        pl.semaphore_wait(nbr.at[1], 1)

        @pl.when(z >= 1)
        def _():
            pl.semaphore_wait(nbr.at[2], 1)

        @pl.when(z <= 2)
        def _():
            pl.semaphore_wait(nbr.at[3], 1)

    get_tab = pltpu.make_async_copy(tab, ev, sem_in.at[4])
    get_tab.start()
    for half in range(2):
        load_x(0, half).start()
    acc[...] = jnp.zeros_like(acc)
    tacc[...] = jnp.zeros_like(tacc)
    dgacc[...] = jnp.zeros_like(dgacc)
    get_tab.wait()
    last = n_chunks + DEPTH

    def iteration(i, _):
        s = i - 1
        busy = in_range(s)
        ahead = i < n_chunks
        scope = jax.named_scope

        with scope("stat"):
            @pl.when(busy)
            def _():
                wait(swap32(st, s % 2, sem_st))

        with scope("dz"):
            @pl.when(busy)
            def _():
                lse = merge(st, s % 2, 32)
                tacc[0:1, :] += wgt[pl.ds(s, 1), :] * lse
                grad_logits(s, lse)

        with scope("xwait"):
            @pl.when(ahead)
            def _():
                for half in range(2):
                    load_x(i, half).wait()

        with scope("norm"):
            @pl.when(ahead)
            def _():
                norm(i)

        with scope("logits"):
            @pl.when(ahead)
            def _():
                top = logits(i)
                st[i % 2, 0] = local_lse(i, top)

        with scope("hear"):
            @pl.when(ahead)
            def _():
                start(swap32(st, i % 2, sem_st))

            @pl.when(i >= 2)
            def _():
                hear_neighbours()

        with scope("partner"):
            @pl.when(in_range(s - 1))
            def _():
                add_partner(s - 1)

        with scope("serve_a"):
            serve_two(s, "x", 0, COL_A, r1a, zra, zla, fsa, fka, r3a, sem_a["1"], sem_a["z"], sem_a["3"])

        with scope("serve_b"):
            serve_two(s, "y", COL_A, COL_B, r1b, zrb, zlb, fsb, fkb, r3b, sem_b["1"], sem_b["z"], sem_b["3"])

        with scope("serve_c"):
            serve_c(s)

        with scope("tell"):
            @pl.when((i >= 1) & (i < last))
            def _():
                tell_neighbours()

        with scope("finish"):
            k = s - 5

            @pl.when(in_range(k))
            def _():
                load_own(k).start()

            @pl.when(in_range(k - 1))
            def _():
                finish(k - 1)

        with scope("de"):
            @pl.when(busy & (s < n_chunks - 1))
            def _():
                embed_grad(s)

            @pl.when(i + 1 < n_chunks)
            def _():
                for half in range(2):
                    load_x(i + 1, half).start()

        with scope("dh"):
            @pl.when(busy)
            def _():
                hidden_grad(s)

        with scope("de_last"):
            @pl.when(s == n_chunks - 1)
            def _():
                embed_grad(s)

        with scope("store"):
            @pl.when(i == n_chunks)
            def _():
                pltpu.make_async_copy(acc, de_out, sem_out.at[2]).start()

        return 0

    lax.fori_loop(0, last + 1, iteration, 0)
    dg1[0, 0, :, 0:width] = jnp.sum(dgacc[...], axis=0, keepdims=True)
    dg1[0, 0, :, width : width + ROWS] = tacc[1:2, :]
    start(swap8(dg1, 0, sem_g1))
    wait(swap8(dg1, 0, sem_g1))
    dg2[0, 0] = sum(dg1[0, q] for q in range(8))
    start(swap4(dg2, 0, sem_g2))
    wait(swap4(dg2, 0, sem_g2))
    total = sum(dg2[0, q] for q in range(4))
    dg_out[...] = total[:, 0:width]
    loss_out[...] = tacc[0:1, :] - total[:, width : width + ROWS]
    for n in (n_chunks - 2, n_chunks - 1):
        store_dx(n).wait()
    pltpu.make_async_copy(acc, de_out, sem_out.at[2]).wait()


def solution(mesh):
    def local_step(residual, labels, loss_mask, norm_gain, table_shard):
        tokens, width = residual.shape
        vocab = table_shard.shape[0]
        n_chunks = tokens // ROWS
        f32, bf16 = jnp.float32, jnp.bfloat16

        def by_chunk(v):
            return v.reshape(16, 2, n_chunks, GROUP).transpose(2, 1, 0, 3).reshape(n_chunks, ROWS)

        weight = loss_mask / jnp.sum(loss_mask)
        dma = pltpu.SemaphoreType.DMA
        vm = pltpu.VMEM
        scratch = [
            vm((vocab, width), bf16), vm((2, 32, GROUP, width), bf16),
            vm((vocab, ROWS), f32), vm((vocab, ROWS), bf16), vm((ROWS, vocab), bf16),
            vm((vocab, width), f32), vm((3, 4, 2, 2, 8, width), f32), vm((4, 2, 2, 8, width), f32),
            vm((5, 4, 2, 8, COL_A), f32), vm((5, 4, 2, 8, COL_B), f32),
            vm((3, 4, 2, 8, COL_C), f32), vm((5, 4, 8, COL_C), f32),
            vm((3, 3, 2, 8, COL_A), f32), vm((3, 3, 2, 8, COL_A), f32),
            vm((3, 3, 2, 8, COL_B), f32), vm((3, 3, 2, 8, COL_B), f32),
            vm((3, 3, 8, COL_C), f32), vm((3, 3, 8, COL_C), f32),
            vm((8, COL_A), f32), vm((8, COL_A), f32), vm((2, 8, COL_A), f32),
            vm((8, COL_B), f32), vm((8, COL_B), f32), vm((2, 8, COL_B), f32),
            vm((2, 32, 1, ROWS), f32), vm((8, ROWS), f32), vm((32, 8, 128), f32),
            vm((8, width), f32), vm((2, 8, width), bf16), vm((2, 8, width), f32), vm((8, width), f32),
            vm((1, 8, 1, width + ROWS), f32), vm((1, 4, 1, width + ROWS), f32),
            dma((5,)), dma((3,)), dma((2, 2)), pltpu.SemaphoreType.REGULAR, pltpu.SemaphoreType.REGULAR((4,)),
            dma((2, 2, 32)), dma((2, 1, 8)), dma((2, 1, 4)),
            {"1": dma((2, 2)), "z": dma((2, 2, 3, 2)), "3": dma((2, 2))},
            {"1": dma((2, 2)), "z": dma((2, 2, 3, 2)), "3": dma((2, 2))},
            {"1": dma((2, 2)), "z": dma((2, 2, 3, 2)), "2": dma((2, 2))},
        ]
        whole = pl.BlockSpec(memory_space=pltpu.VMEM)
        raw = pl.BlockSpec(memory_space=pl.ANY)
        dx, de, dg, loss = pl.pallas_call(
            functools.partial(step_kernel, n_chunks),
            out_shape=(
                jax.ShapeDtypeStruct((n_chunks, GROUP, width), f32),
                jax.ShapeDtypeStruct((vocab, width), f32),
                jax.ShapeDtypeStruct((1, width), f32),
                jax.ShapeDtypeStruct((1, ROWS), f32),
            ),
            in_specs=[raw, whole, whole, whole, raw],
            out_specs=(raw, raw, whole, whole),
            scratch_shapes=scratch,
            compiler_params=pltpu.CompilerParams(vmem_limit_bytes=67043328, has_side_effects=True),
            name="head_step",
        )(
            residual.reshape(16, 2, n_chunks, GROUP, width),
            by_chunk(labels),
            by_chunk(weight),
            norm_gain.reshape(1, width),
            table_shard,
        )
        return jnp.sum(loss), dx.reshape(n_chunks * GROUP, width), de / LOGIT_SCALE, dg.reshape(width)

    return jax.shard_map(local_step, mesh=mesh, in_specs=(P(), P(), P(), P(), P("vp", None)), out_specs=(P(), P("vp", None), P("vp", None), P()), check_vma=False)
```

```python
import functools

import jax
import jax.numpy as jnp
from jax import lax
from jax.experimental import pallas as pl
from jax.experimental.pallas import tpu as pltpu
from jax.sharding import PartitionSpec as P

VOCAB_REAL = 49155
LOGIT_SCALE = 6.0
NORM_EPS = 1e-6
MESH = pl.DeviceIdType.MESH

GROUP = 8
ROWS = 32 * GROUP
COL_A, COL_B, COL_C = 896, 1792, 1408
DEPTH = 6
VMEM_LIMIT = 67043328
GRID = (4, 2, 2)


def step_kernel(
    n_chunks, res, tok, gain, tab,
    dx_out, de_out, dg_out, loss_out,
    ev, h, zt, dzt, dz, acc, op, r0,
    r1a, r1b, r1c, r2c, zra, zla, zrb, zlb, zrc, zlc,
    fsa, fka, r3a, fsb, fkb, r3b,
    st, tacc, ssq, dhf, xr, dxb, dgacc, dg1, dg2,
    sem_in, sem_tab, sem_out, sem_p, cred, nbr, sem_st, sem_g1, sem_g2,
    sem_a, sem_b, sem_c,
):
    vocab, width = ev.shape
    edges = list(range(0, max(vocab - 511, 1), 512)) + [vocab]
    blocks = [(a, b - a) for a, b in zip(edges, edges[1:])]
    me = lax.axis_index("vp")
    c, x, y, z = me % 2, (me // 2) % 2, (me // 4) % 2, me // 8

    def dev(zz, yy, xx, cc):
        return (((zz * 2 + yy) * 2 + xx) * 2 + cc,)

    def send(src, dst, ssem, rsem, to):
        return pltpu.make_async_remote_copy(src, dst, ssem, rsem, device_id=to, device_id_type=MESH)

    def hop(src, dst, sem, k, to):
        return send(src, dst, sem.at[0, k % 2], sem.at[1, k % 2], to)

    nbr_x, nbr_y = dev(z, y, 1 - x, c), dev(z, 1 - y, x, c)
    nbr_r, nbr_l = dev(z + 1, y, x, c), dev(z - 1, y, x, c)
    partner = dev(z, y, x, 1 - c)

    def load_x(n, half):
        return pltpu.make_async_copy(res.at[:, half, n], h.at[n % 2, pl.ds(16 * half, 16)], sem_in.at[half])

    def tab_block(j):
        a, m = blocks[j]
        return pltpu.make_async_copy(tab.at[pl.ds(a, m)], ev.at[pl.ds(a, m)], sem_tab.at[j])

    def load_own(n):
        return pltpu.make_async_copy(res.at[me // 2, me % 2, n], xr.at[n % 2], sem_in.at[2 + n % 2])

    def store_dx(n):
        return pltpu.make_async_copy(dxb.at[n % 2], dx_out.at[n], sem_out.at[n % 2])

    def label_rows(n):
        return tok[0, pl.ds(n, 1), :].astype(jnp.int32) - me * vocab

    def weights(n):
        return tok[1, pl.ds(n, 1), :] / tacc[2:3, :]

    def norm(n):
        slot = n % 2
        pieces = range(0, width, 256)

        def piece(i, j):
            return h[slot, i, :, j : j + 256].astype(jnp.float32)

        def squares(i, _):
            parts = []
            for j in pieces:
                sq = piece(i, j)
                sq = sq * sq
                parts.append(sq[:, :128] + sq[:, 128:])
            while len(parts) > 1:
                parts = [p + q for p, q in zip(parts[::2], parts[1::2])]
            ssq[i] = parts[0]
            return 0

        def scale(i, _):
            inv = jnp.concatenate([ssq[i], ssq[i]], axis=1)
            for j in pieces:
                h[slot, i, :, j : j + 256] = ((piece(i, j) * inv) * gain[:, j : j + 256]).astype(jnp.bfloat16)
            return 0

        lax.fori_loop(0, 32, squares, 0, unroll=4)
        mean = jnp.sum(ssq[...], axis=-1, keepdims=True) * (1.0 / width)
        ssq[...] = jnp.broadcast_to(lax.rsqrt(mean + NORM_EPS), ssq.shape)
        lax.fori_loop(0, 32, scale, 0, unroll=4)

    def logits(n):
        top = jnp.full((1, ROWS), -jnp.inf, jnp.float32)
        hn = h[n % 2].reshape(ROWS, width)
        for a, m in blocks:
            t = lax.dot_general(ev[a : a + m, :], hn, (((1,), (1,)), ((), ())), preferred_element_type=jnp.float32)
            t = t * (1.0 / LOGIT_SCALE)
            ids = me * vocab + a + lax.broadcasted_iota(jnp.int32, (m, ROWS), 0)
            t = jnp.where(ids < VOCAB_REAL, t, -jnp.inf)
            zt[a : a + m, :] = t
            top = jnp.maximum(top, jnp.max(t, axis=0, keepdims=True))
        return top

    full_tiles = vocab // 128
    tail = vocab - full_tiles * 128

    def local_lse(n, top):
        lb = label_rows(n)

        def part(a, m, s, t):
            v = zt[pl.ds(a, m), :]
            ids = a + lax.broadcasted_iota(jnp.int32, (m, ROWS), 0)
            e = jnp.exp(v - top).reshape(m // 8, 8, ROWS)
            hit = jnp.where(ids == lb, v, 0.0).reshape(m // 8, 8, ROWS)
            return s + jnp.sum(e, axis=0), t + jnp.sum(hit, axis=0)

        zero = jnp.zeros((8, ROWS), jnp.float32)
        s, t = lax.fori_loop(0, full_tiles, lambda i, v: part(pl.multiple_of(i * 128, 128), 128, *v), (zero, zero))
        s, t = part(full_tiles * 128, tail, s, t)
        tacc[1:2, :] += weights(n) * jnp.sum(t, axis=0, keepdims=True)
        return top + jnp.log(jnp.sum(s, axis=0, keepdims=True))

    def merge(ref, slot, count):
        rows = [ref[slot, q] for q in range(count)]
        top = functools.reduce(jnp.maximum, rows)
        return top + jnp.log(sum(jnp.exp(r - top) for r in rows))

    def grad_logits(k, lse):
        lb = label_rows(k)
        w = weights(k)
        for a, m in [(i * 128, 128) for i in range(full_tiles)] + [(full_tiles * 128, tail)]:
            ids = a + lax.broadcasted_iota(jnp.int32, (m, ROWS), 0)
            p = jnp.exp(zt[a : a + m, :] - lse)
            d = (jnp.where(ids == lb, p - 1.0, p) * w).astype(jnp.bfloat16)
            dzt[a : a + m, :] = d
            dz[:, a : a + m] = d.T

    def embed_grad(k):
        tile = width // 4
        for a, m in blocks:
            for j in range(4):
                cols = pl.ds(j * tile, tile)
                acc[a : a + m, cols] += jnp.dot(dzt[a : a + m, :], h[k % 2, :, :, cols].reshape(ROWS, tile), preferred_element_type=jnp.float32)

    def send_p(half):
        cols = pl.ds(half * (width // 2), width // 2)
        return send(op.at[2, :, :, :, :, cols], r0.at[:, :, :, :, cols], sem_p.at[0, half], sem_p.at[1, half], partner)

    def hidden_grad(k):
        own = k % 2
        eq0 = 1 - c
        where = (eq0 * own + (1 - eq0) * 2, c * own + (1 - c) * 2)
        for half in range(2):
            cols = pl.ds(half * (width // 2), width // 2)
            r = jnp.dot(dz[...], ev[:, cols], preferred_element_type=jnp.float32)
            for q in range(2):
                op[where[q], :, :, :, :, cols] = r[q * 128 : (q + 1) * 128].reshape(4, 2, 2, 8, width // 2)
            if half == 0:
                @pl.when(k >= 1)
                def _():
                    pl.semaphore_wait(cred, 1)
            send_p(half).start()

    def add_partner(k):
        for half in range(2):
            send_p(half).wait()

        def body(i, _):
            op[k % 2, i] += r0[i]
            return 0

        lax.fori_loop(0, 4, body, 0)

        @pl.when(k < n_chunks - 1)
        def _():
            pl.semaphore_signal(cred, 1, device_id=partner, device_id_type=MESH)

    def peer(q):
        qy, qx, qc = (q // 4) % 2, (q // 2) % 2, q % 2
        return dev((z + q // 8) % 4, y + qy * (1 - 2 * y), x + qx * (1 - 2 * x), c + qc * (1 - 2 * c))

    def swap8(buf, slot, sem):
        return [send(buf.at[slot, 0], buf.at[slot, q], sem.at[0, slot, q], sem.at[1, slot, q], peer(q)) for q in range(1, 8)]

    def swap32(buf, slot, sem):
        out = []
        for q in range(1, 32):
            there = ((4 - q // 8) % 4) * 8 + q % 8
            out.append(send(buf.at[slot, 0], buf.at[slot, there], sem.at[0, slot, q], sem.at[1, slot, there], peer(q)))
        return out

    def swap4(buf, slot, sem):
        return [
            send(buf.at[slot, 0], buf.at[slot, 4 - q], sem.at[0, slot, q], sem.at[1, slot, 4 - q], peer(8 * q))
            for q in range(1, 4)
        ]

    def start(copies):
        for cp in copies:
            cp.start()

    def wait(copies):
        for cp in copies:
            cp.wait_send()
        for cp in copies:
            cp.wait_recv()

    def z_copies(zr, zl, s1, sl, t, zslot, sem, par):
        ways = []
        for way, (buf, to, block) in enumerate(((zr, nbr_r, 3 - t), (zl, nbr_l, t))):
            sems = (sem.at[0, way, t, par], sem.at[1, way, t, par])
            first = send(s1.at[sl, block], buf.at[t, zslot], *sems, to)
            later = send(buf.at[t - 1, zslot], buf.at[t, zslot], *sems, to) if t else None
            behind, ahead = (z, 3 - z) if way == 0 else (3 - z, z)
            ways.append((behind, ahead, first, later))
        return ways

    def z_wait(ways, t):
        for behind, ahead, first, _ in ways:
            @pl.when((behind <= t) & (ahead > 0))
            def _(first=first):
                first.wait_send()

            @pl.when((behind > 0) & (behind <= t + 1))
            def _(first=first):
                first.wait_recv()

    def z_start(ways, zr, zl, s1, sl, t, zslot):
        for (behind, ahead, first, later), buf, block in zip(ways, (zr, zl), (3 - t + z, t - 3 + z)):
            @pl.when(behind == 0)
            def _(first=first):
                first.start()

            if t:
                @pl.when((behind > 0) & (behind <= t) & (ahead > 0))
                def _(buf=buf, block=block, later=later):
                    buf[t - 1, zslot] += s1[sl, block]
                    later.start()

    def in_range(k):
        return (k >= 0) & (k < n_chunks)

    def serve_two(s, axis, col, size, r1, zr, zl, fs, fk, r3, sem):
        cols = pl.ds(col, size)
        first_nbr, last_nbr = (nbr_x, nbr_y) if axis == "x" else (nbr_y, nbr_x)
        q = y if axis == "x" else x

        def copy1(k):
            src = op.at[k % 2, :, :, 1 - x, :, cols] if axis == "x" else op.at[k % 2, :, 1 - y, :, :, cols]
            return hop(src, r1.at[k % 5], sem["first"], k, first_nbr)

        def copy3(k):
            return hop(fs, r3.at[k % 2], sem["last"], k, last_nbr)

        def zc(k, t):
            return z_copies(zr, zl, r1, k % 5, t, k % 3, sem["z"], k % 2)

        k = s - 6

        @pl.when(in_range(k))
        def _():
            copy3(k).wait()
            dhf[:, cols] = fk[...] + r3[k % 2]

        k5 = s - 5

        @pl.when(in_range(k5))
        def _():
            z_wait(zc(k5, 2), 2)
            sl = k5 % 5
            fs[...] = r1[sl, z, 1 - q]
            fk[...] = r1[sl, z, q]

            @pl.when(z >= 1)
            def _():
                fs[...] += zr[2, k5 % 3, 1 - q]
                fk[...] += zr[2, k5 % 3, q]

            @pl.when(z <= 2)
            def _():
                fs[...] += zl[2, k5 % 3, 1 - q]
                fk[...] += zl[2, k5 % 3, q]

            copy3(k5).start()

        for t, back in ((2, 4), (1, 3)):
            kt = s - back

            @pl.when(in_range(kt))
            def _(kt=kt, t=t):
                z_wait(zc(kt, t - 1), t - 1)
                z_start(zc(kt, t), zr, zl, r1, kt % 5, t, kt % 3)

        k2 = s - 2

        @pl.when(in_range(k2))
        def _():
            copy1(k2).wait()
            for b in range(4):
                kept = op[k2 % 2, b, :, x, :, cols] if axis == "x" else op[k2 % 2, b, y, :, :, cols]
                r1[k2 % 5, b] += kept
            z_start(zc(k2, 0), zr, zl, r1, k2 % 5, 0, k2 % 3)

        k1 = s - 1

        @pl.when(in_range(k1))
        def _():
            copy1(k1).start()

    def serve_c(s):
        cols = pl.ds(COL_A + COL_B, COL_C)

        def copy1(k):
            return hop(op.at[k % 2, :, :, 1 - x, :, cols], r1c.at[k % 3], sem_c["first"], k, nbr_x)

        def copy2(k):
            return hop(r1c.at[k % 3, :, 1 - y], r2c.at[k % 5], sem_c["last"], k, nbr_y)

        def zc(k, t):
            return z_copies(zrc, zlc, r2c, k % 5, t, k % 3, sem_c["z"], k % 2)

        k = s - 6

        @pl.when(in_range(k))
        def _():
            z_wait(zc(k, 2), 2)
            dhf[:, cols] = r2c[k % 5, z]

            @pl.when(z >= 1)
            def _():
                dhf[:, cols] += zrc[2, k % 3]

            @pl.when(z <= 2)
            def _():
                dhf[:, cols] += zlc[2, k % 3]

        for t, back in ((2, 5), (1, 4)):
            kt = s - back

            @pl.when(in_range(kt))
            def _(kt=kt, t=t):
                z_wait(zc(kt, t - 1), t - 1)
                z_start(zc(kt, t), zrc, zlc, r2c, kt % 5, t, kt % 3)

        k3 = s - 3

        @pl.when(in_range(k3))
        def _():
            copy2(k3).wait()
            for b in range(4):
                r2c[k3 % 5, b] += r1c[k3 % 3, b, y]
            z_start(zc(k3, 0), zrc, zlc, r2c, k3 % 5, 0, k3 % 3)

        k2 = s - 2

        @pl.when(in_range(k2))
        def _():
            copy1(k2).wait()
            for b in range(4):
                r1c[k2 % 3, b] += op[k2 % 2, b, :, x, :, cols]
            copy2(k2).start()

        k1 = s - 1

        @pl.when(in_range(k1))
        def _():
            copy1(k1).start()

    def finish(k):
        load_own(k).wait()

        @pl.when(k >= 2)
        def _():
            store_dx(k - 2).wait()

        xo = xr[k % 2].astype(jnp.float32)
        inv = lax.rsqrt(jnp.mean(xo * xo, axis=-1, keepdims=True) + NORM_EPS)
        xh = xo * inv
        dh = dhf[...] / LOGIT_SCALE
        dgacc[...] += dh * xh
        u = dh * gain[...]
        dxb[k % 2] = inv * (u - xh * jnp.mean(u * xh, axis=-1, keepdims=True))
        store_dx(k).start()

    def tell_neighbours():
        pl.semaphore_signal(nbr.at[0], 1, device_id=nbr_x, device_id_type=MESH)
        pl.semaphore_signal(nbr.at[1], 1, device_id=nbr_y, device_id_type=MESH)

        @pl.when(z <= 2)
        def _():
            pl.semaphore_signal(nbr.at[2], 1, device_id=nbr_r, device_id_type=MESH)

        @pl.when(z >= 1)
        def _():
            pl.semaphore_signal(nbr.at[3], 1, device_id=nbr_l, device_id_type=MESH)

    def hear_neighbours():
        pl.semaphore_wait(nbr.at[0], 1)
        pl.semaphore_wait(nbr.at[1], 1)

        @pl.when(z >= 1)
        def _():
            pl.semaphore_wait(nbr.at[2], 1)

        @pl.when(z <= 2)
        def _():
            pl.semaphore_wait(nbr.at[3], 1)

    with jax.named_scope("init"):
        for half in range(2):
            load_x(0, half).start()
        for j in range(len(blocks)):
            tab_block(j).start()
        barrier = pltpu.get_barrier_semaphore()
        for q in range(1, 32):
            pl.semaphore_signal(barrier, 1, device_id=peer(q), device_id_type=MESH)
        tacc[...] = jnp.zeros_like(tacc)
        tacc[2:3, :] = jnp.broadcast_to(jnp.sum(tok[1], keepdims=True), (1, ROWS))
        dgacc[...] = jnp.zeros_like(dgacc)
    last = n_chunks + DEPTH

    def iteration(i, _):
        s = i - 1
        busy = in_range(s)
        ahead = i < n_chunks
        scope = jax.named_scope

        with scope("xwait"):
            @pl.when(ahead)
            def _():
                for half in range(2):
                    load_x(i, half).wait()

        with scope("norm"):
            @pl.when(ahead)
            def _():
                norm(i)

        with scope("stat"):
            @pl.when(busy)
            def _():
                wait(swap32(st, s % 2, sem_st))

        with scope("dz"):
            @pl.when(busy)
            def _():
                lse = merge(st, s % 2, 32)
                tacc[0:1, :] += weights(s) * lse
                grad_logits(s, lse)

        with scope("tabwait"):
            @pl.when(i == 0)
            def _():
                for j in range(len(blocks)):
                    tab_block(j).wait()

        with scope("logits"):
            @pl.when(ahead)
            def _():
                top = logits(i)
                st[i % 2, 0] = local_lse(i, top)

        with scope("meet"):
            @pl.when(i == 0)
            def _():
                pl.semaphore_wait(barrier, 31)

        with scope("hear"):
            @pl.when(ahead)
            def _():
                start(swap32(st, i % 2, sem_st))

            @pl.when(i >= 2)
            def _():
                hear_neighbours()

        with scope("partner"):
            @pl.when(in_range(s - 1))
            def _():
                add_partner(s - 1)

        with scope("serve_a"):
            serve_two(s, "x", 0, COL_A, r1a, zra, zla, fsa, fka, r3a, sem_a)

        with scope("serve_b"):
            serve_two(s, "y", COL_A, COL_B, r1b, zrb, zlb, fsb, fkb, r3b, sem_b)

        with scope("serve_c"):
            serve_c(s)

        with scope("tell"):
            @pl.when((i >= 1) & (i < last))
            def _():
                tell_neighbours()

        with scope("finish"):
            k = s - 5

            @pl.when(in_range(k))
            def _():
                load_own(k).start()

            @pl.when(in_range(k - 1))
            def _():
                finish(k - 1)

        with scope("de_last"):
            @pl.when(s == n_chunks)
            def _():
                embed_grad(s - 1)
                acc[...] = acc[...] * (1.0 / LOGIT_SCALE)
                pltpu.make_async_copy(acc, de_out, sem_out.at[2]).start()

        with scope("zero"):
            @pl.when(i == 0)
            def _():
                acc[...] = jnp.zeros_like(acc)

        with scope("de"):
            @pl.when(busy & (s < n_chunks - 1))
            def _():
                embed_grad(s)

            @pl.when(i + 1 < n_chunks)
            def _():
                for half in range(2):
                    load_x(i + 1, half).start()

        with scope("dh"):
            @pl.when(busy)
            def _():
                hidden_grad(s)

        return 0

    lax.fori_loop(0, last + 1, iteration, 0)
    with jax.named_scope("gain"):
        dg1[0, 0, :, 0:width] = jnp.sum(dgacc[...], axis=0, keepdims=True)
        dg1[0, 0, :, width : width + ROWS] = tacc[1:2, :]
        start(swap8(dg1, 0, sem_g1))
        wait(swap8(dg1, 0, sem_g1))
        dg2[0, 0] = sum(dg1[0, q] for q in range(8))
        start(swap4(dg2, 0, sem_g2))
        wait(swap4(dg2, 0, sem_g2))
        total = sum(dg2[0, q] for q in range(4))
        dg_out[...] = total[:, 0:width]
        loss_out[...] = tacc[0:1, :] - total[:, width : width + ROWS]
        for n in (n_chunks - 2, n_chunks - 1):
            store_dx(n).wait()
        pltpu.make_async_copy(acc, de_out, sem_out.at[2]).wait()


def hand_over_kernel(de_in, dx_in, dg_in, loss_in, de_out, dx_out, dg_out, loss_out, buf, sem):
    step = buf.shape[1]
    gets, puts = [], []
    for src, dst in ((de_in, de_out), (dx_in, dx_out)):
        rows = src.shape[0]
        for r in range(0, rows, step):
            n, some = len(gets), pl.ds(r, min(step, rows - r))
            here = buf.at[n, pl.ds(0, some.size)]
            gets.append(pltpu.make_async_copy(src.at[some], here, sem.at[0, n]))
            puts.append(pltpu.make_async_copy(here, dst.at[some], sem.at[1, n]))
    for get in gets:
        get.start()
    dg_out[...] = dg_in[...]
    loss_out[...] = jnp.sum(loss_in[...], keepdims=True)
    for get, put in zip(gets, puts):
        get.wait()
    for put in puts:
        put.start()
    for put in puts:
        put.wait()


def solution(mesh):
    def local_step(residual, labels, loss_mask, norm_gain, table_shard):
        tokens, width = residual.shape
        vocab = table_shard.shape[0]
        n_chunks = tokens // ROWS
        f32, bf16 = jnp.float32, jnp.bfloat16

        tok = jnp.stack([labels.astype(f32), loss_mask]).reshape(2, 16, 2, n_chunks, GROUP)
        tok = tok.transpose(0, 3, 2, 1, 4).reshape(2, n_chunks, ROWS)
        dma = pltpu.SemaphoreType.DMA
        vm = pltpu.VMEM
        slab = (GROUP, width)
        pair, ways = (2, 2), (2, 2, 3, 2)
        scratch = [vm((vocab, width), bf16), vm((2, 32, *slab), bf16), vm((vocab, ROWS), f32)]
        scratch += [vm((vocab, ROWS), bf16), vm((ROWS, vocab), bf16), vm((vocab, width), f32)]
        scratch += [vm((3, *GRID, *slab), f32), vm((*GRID, *slab), f32)]
        scratch += [vm((5, 4, 2, GROUP, n), f32) for n in (COL_A, COL_B)]
        scratch += [vm((3, 4, 2, GROUP, COL_C), f32), vm((5, 4, GROUP, COL_C), f32)]
        for n in (COL_A, COL_B):
            scratch += [vm((3, 3, 2, GROUP, n), f32)] * 2
        scratch += [vm((3, 3, GROUP, COL_C), f32)] * 2
        for n in (COL_A, COL_B):
            scratch += [vm((GROUP, n), f32), vm((GROUP, n), f32), vm((2, GROUP, n), f32)]
        scratch += [vm((2, 32, 1, ROWS), f32), vm((GROUP, ROWS), f32), vm((32, GROUP, 128), f32)]
        scratch += [vm(slab, f32), vm((2, *slab), bf16), vm((2, *slab), f32), vm(slab, f32)]
        scratch += [vm((1, n, 1, width + ROWS), f32) for n in (8, 4)]
        scratch += [dma((4,)), dma((8,)), dma((3,)), dma(pair), pltpu.SemaphoreType.REGULAR, pltpu.SemaphoreType.REGULAR((4,))]
        scratch += [dma((2, 2, 32)), dma((2, 1, 8)), dma((2, 1, 4))]
        scratch += [{"first": dma(pair), "z": dma(ways), "last": dma(pair)}] * 3
        whole = pl.BlockSpec(memory_space=pltpu.VMEM)
        raw = pl.BlockSpec(memory_space=pl.ANY)
        dx, de, dg, loss = pl.pallas_call(
            functools.partial(step_kernel, n_chunks),
            out_shape=(
                jax.ShapeDtypeStruct((n_chunks, GROUP, width), f32),
                jax.ShapeDtypeStruct((vocab, width), f32),
                jax.ShapeDtypeStruct((1, width), f32),
                jax.ShapeDtypeStruct((1, ROWS), f32),
            ),
            in_specs=[raw, whole, whole, raw],
            out_specs=(raw, raw, whole, whole),
            scratch_shapes=scratch,
            compiler_params=pltpu.CompilerParams(vmem_limit_bytes=VMEM_LIMIT, has_side_effects=True, collective_id=0),
            name="head_step",
        )(
            residual.reshape(16, 2, n_chunks, GROUP, width),
            tok,
            norm_gain.reshape(1, width),
            table_shard,
        )
        de, dx, dg, loss = pl.pallas_call(
            hand_over_kernel,
            out_shape=(
                jax.ShapeDtypeStruct((vocab, width), f32),
                jax.ShapeDtypeStruct((n_chunks * GROUP, width), f32),
                jax.ShapeDtypeStruct((1, width), f32),
                jax.ShapeDtypeStruct((1, 1), f32),
            ),
            in_specs=[raw, raw, whole, whole],
            out_specs=(raw, raw, whole, whole),
            scratch_shapes=[vm((16, 128, width), f32), dma((2, 16))],
            compiler_params=pltpu.CompilerParams(vmem_limit_bytes=VMEM_LIMIT),
            name="hand_over",
        )(de, dx.reshape(n_chunks * GROUP, width), dg, loss)
        return loss.reshape(()), dx, de, dg.reshape(width)

    return jax.shard_map(local_step, mesh=mesh, in_specs=(P(), P(), P(), P(), P("vp", None)), out_specs=(P(), P("vp", None), P("vp", None), P()), check_vma=False)
```

```python
import functools

import jax
import jax.numpy as jnp
from jax import lax
from jax.experimental import pallas as pl
from jax.experimental.pallas import tpu as pltpu
from jax.sharding import PartitionSpec as P

VOCAB_REAL = 49155
LOGIT_SCALE = 6.0
NORM_EPS = 1e-6
MESH = pl.DeviceIdType.MESH

GROUP = 8
ROWS = 32 * GROUP
COL_A, COL_B, COL_C = 896, 1792, 1408
DEPTH = 3
VMEM_LIMIT = 67043328
GRID = (4, 2, 2)


def step_kernel(
    n_chunks, res, tok, gain, tab,
    dx_out, de_out, sums_out,
    ev, h, zt, dzt, dz, acc, op, r0,
    r1a, r1b, r1c, r2c, zra, zla, zrb, zlb, zrc, zlc,
    fsa, fka, r3a, fsb, fkb, r3b,
    st, tacc, ssq, dhf, xr, dxb, dgacc, dg1, dg2,
    sem_in, sem_tab, sem_out, sem_p, cred, nbr, sem_st, sem_g1, sem_g2,
    sem_a, sem_b, sem_c,
):
    vocab, width = ev.shape
    edges = list(range(0, max(vocab - 511, 1), 512)) + [vocab]
    blocks = [(a, b - a) for a, b in zip(edges, edges[1:])]
    me = lax.axis_index("vp")
    c, x, y, z = me % 2, (me // 2) % 2, (me // 4) % 2, me // 8

    def dev(zz, yy, xx, cc):
        return (((zz * 2 + yy) * 2 + xx) * 2 + cc,)

    def send(src, dst, ssem, rsem, to):
        return pltpu.make_async_remote_copy(src, dst, ssem, rsem, device_id=to, device_id_type=MESH)

    def hop(src, dst, sem, k, to):
        return send(src, dst, sem.at[0, k % 2], sem.at[1, k % 2], to)

    nbr_x, nbr_y = dev(z, y, 1 - x, c), dev(z, 1 - y, x, c)
    nbr_r, nbr_l = dev(z + 1, y, x, c), dev(z - 1, y, x, c)
    partner = dev(z, y, x, 1 - c)

    def load_x(n, half):
        return pltpu.make_async_copy(res.at[:, half, n], h.at[n % 3, pl.ds(16 * half, 16)], sem_in.at[half])

    def tab_block(j):
        a, m = blocks[j]
        return pltpu.make_async_copy(tab.at[pl.ds(a, m)], ev.at[pl.ds(a, m)], sem_tab.at[j])

    def load_own(n):
        return pltpu.make_async_copy(res.at[me // 2, me % 2, n], xr.at[n % 2], sem_in.at[2 + n % 2])

    def store_dx(n):
        return pltpu.make_async_copy(dxb.at[n % 2], dx_out.at[n], sem_out.at[n % 2])

    def label_rows(n):
        return tok[0, pl.ds(n, 1), :].astype(jnp.int32) - me * vocab

    def weights(n):
        return tok[1, pl.ds(n, 1), :] / tacc[2:3, :]

    def norm(n):
        slot = n % 3
        pieces = range(0, width, 256)

        def piece(i, j):
            return h[slot, i, :, j : j + 256].astype(jnp.float32)

        def squares(i, _):
            parts = []
            for j in pieces:
                sq = piece(i, j)
                sq = sq * sq
                parts.append(sq[:, :128] + sq[:, 128:])
            while len(parts) > 1:
                parts = [p + q for p, q in zip(parts[::2], parts[1::2])]
            ssq[i] = parts[0]
            return 0

        def scale(i, _):
            inv = jnp.concatenate([ssq[i], ssq[i]], axis=1)
            for j in pieces:
                h[slot, i, :, j : j + 256] = ((piece(i, j) * inv) * gain[:, j : j + 256]).astype(jnp.bfloat16)
            return 0

        lax.fori_loop(0, 32, squares, 0, unroll=8)
        mean = jnp.sum(ssq[...], axis=-1, keepdims=True) * (1.0 / width)
        ssq[...] = jnp.broadcast_to(lax.rsqrt(mean + NORM_EPS), ssq.shape)
        lax.fori_loop(0, 32, scale, 0, unroll=8)

    def logits(n):
        top = jnp.full((1, ROWS), -jnp.inf, jnp.float32)
        hn = h[n % 3].reshape(ROWS, width)
        for a, m in blocks:
            t = lax.dot_general(ev[a : a + m, :], hn, (((1,), (1,)), ((), ())), preferred_element_type=jnp.float32)
            t = t * (1.0 / LOGIT_SCALE)
            ids = me * vocab + a + lax.broadcasted_iota(jnp.int32, (m, ROWS), 0)
            t = jnp.where(ids < VOCAB_REAL, t, -jnp.inf)
            zt[a : a + m, :] = t
            top = jnp.maximum(top, jnp.max(t, axis=0, keepdims=True))
        return top

    full_tiles = vocab // 128
    tail = vocab - full_tiles * 128

    def local_lse(n, top):
        lb = label_rows(n)

        def part(a, m, s, t):
            v = zt[pl.ds(a, m), :]
            ids = a + lax.broadcasted_iota(jnp.int32, (m, ROWS), 0)
            e = jnp.exp(v - top).reshape(m // 8, 8, ROWS)
            hit = jnp.where(ids == lb, v, 0.0).reshape(m // 8, 8, ROWS)
            return s + jnp.sum(e, axis=0), t + jnp.sum(hit, axis=0)

        zero = jnp.zeros((8, ROWS), jnp.float32)
        s, t = lax.fori_loop(0, full_tiles, lambda i, v: part(pl.multiple_of(i * 128, 128), 128, *v), (zero, zero))
        s, t = part(full_tiles * 128, tail, s, t)
        tacc[1:2, :] += weights(n) * jnp.sum(t, axis=0, keepdims=True)
        return top + jnp.log(jnp.sum(s, axis=0, keepdims=True))

    def merge(ref, slot, count):
        rows = [ref[slot, q] for q in range(count)]
        top = functools.reduce(jnp.maximum, rows)
        return top + jnp.log(sum(jnp.exp(r - top) for r in rows))

    def grad_logits(k, lse):
        lb = label_rows(k)
        w = weights(k)
        for a, m in [(i * 128, 128) for i in range(full_tiles)] + [(full_tiles * 128, tail)]:
            ids = a + lax.broadcasted_iota(jnp.int32, (m, ROWS), 0)
            p = jnp.exp(zt[a : a + m, :] - lse)
            d = (jnp.where(ids == lb, p - 1.0, p) * w).astype(jnp.bfloat16)
            dzt[a : a + m, :] = d
            dz[:, a : a + m] = d.T

    def embed_grad(k, half):
        tile = width // 4
        for a, m in blocks:
            for j in (2 * half, 2 * half + 1):
                cols = pl.ds(j * tile, tile)
                acc[a : a + m, cols] += jnp.dot(dzt[a : a + m, :], h[k % 3, :, :, cols].reshape(ROWS, tile), preferred_element_type=jnp.float32)

    split = width * 3 // 4
    parts = (pl.ds(0, split), pl.ds(split, width - split))

    def send_p(part):
        cols = parts[part]
        return send(op.at[2, :, :, :, :, cols], r0.at[:, :, :, :, cols], sem_p.at[0, part], sem_p.at[1, part], partner)

    def hidden_grad(k, part):
        own = k % 2
        where = ((1 - c) * own + c * 2, c * own + (1 - c) * 2)
        cols = parts[part]
        r = jnp.dot(dz[...], ev[:, cols], preferred_element_type=jnp.float32)
        for q in range(2):
            op[where[q], :, :, :, :, cols] = r[q * 128 : (q + 1) * 128].reshape(4, 2, 2, 8, cols.size)
        if part == 0:
            @pl.when(k >= 1)
            def _():
                pl.semaphore_wait(cred, 1)
        send_p(part).start()

    def add_partner(k):
        for half in range(2):
            send_p(half).wait()

        def body(i, _):
            op[k % 2, i] += r0[i]
            return 0

        lax.fori_loop(0, 4, body, 0)

        @pl.when(k < n_chunks - 1)
        def _():
            pl.semaphore_signal(cred, 1, device_id=partner, device_id_type=MESH)

    def peer(q):
        qy, qx, qc = (q // 4) % 2, (q // 2) % 2, q % 2
        return dev((z + q // 8) % 4, y + qy * (1 - 2 * y), x + qx * (1 - 2 * x), c + qc * (1 - 2 * c))

    def swap8(buf, slot, sem):
        return [send(buf.at[slot, 0], buf.at[slot, q], sem.at[0, slot, q], sem.at[1, slot, q], peer(q)) for q in range(1, 8)]

    def swap32(buf, slot, sem):
        out = []
        for q in range(1, 32):
            there = ((4 - q // 8) % 4) * 8 + q % 8
            out.append(send(buf.at[slot, 0], buf.at[slot, there], sem.at[0, slot, q], sem.at[1, slot, there], peer(q)))
        return out

    def swap4(buf, slot, sem):
        return [
            send(buf.at[slot, 0], buf.at[slot, 4 - q], sem.at[0, slot, q], sem.at[1, slot, 4 - q], peer(8 * q))
            for q in range(1, 4)
        ]

    def start(copies):
        for cp in copies:
            cp.start()

    def wait(copies):
        for cp in copies:
            cp.wait_send()
        for cp in copies:
            cp.wait_recv()

    def z_copies(zr, zl, s1, sl, t, zslot, sem, par):
        ways = []
        for way, (buf, to, block) in enumerate(((zr, nbr_r, 3 - t), (zl, nbr_l, t))):
            sems = (sem.at[0, way, t, par], sem.at[1, way, t, par])
            first = send(s1.at[sl, block], buf.at[t, zslot], *sems, to)
            later = send(buf.at[t - 1, zslot], buf.at[t, zslot], *sems, to) if t else None
            behind, ahead = (z, 3 - z) if way == 0 else (3 - z, z)
            ways.append((behind, ahead, first, later))
        return ways

    def z_wait(ways, t):
        for behind, ahead, first, _ in ways:
            @pl.when((behind <= t) & (ahead > 0))
            def _(first=first):
                first.wait_send()

            @pl.when((behind > 0) & (behind <= t + 1))
            def _(first=first):
                first.wait_recv()

    def z_start(ways, zr, zl, s1, sl, t, zslot):
        for (behind, ahead, first, later), buf, block in zip(ways, (zr, zl), (3 - t + z, t - 3 + z)):
            @pl.when(behind == 0)
            def _(first=first):
                first.start()

            if t:
                @pl.when((behind > 0) & (behind <= t) & (ahead > 0))
                def _(buf=buf, block=block, later=later):
                    buf[t - 1, zslot] += s1[sl, block]
                    later.start()

    def in_range(k):
        return (k >= 0) & (k < n_chunks)

    def two_axes(axis, col, size, r1, zr, zl, fs, fk, r3, sem):
        cols = pl.ds(col, size)
        first_nbr, last_nbr = (nbr_x, nbr_y) if axis == "x" else (nbr_y, nbr_x)
        q = y if axis == "x" else x

        def first(k):
            src = op.at[k % 2, :, :, 1 - x, :, cols] if axis == "x" else op.at[k % 2, :, 1 - y, :, :, cols]
            return hop(src, r1.at[k % 3], sem["first"], k, first_nbr)

        def last_hop(k):
            return hop(fs, r3.at[k % 2], sem["last"], k, last_nbr)

        def zc(k, t):
            return z_copies(zr, zl, r1, k % 3, t, k % 2, sem["z"], k % 2)

        def open_up(s):
            @pl.when(in_range(s))
            def _():
                first(s).start()

        def turn(s):
            k = s - 3

            @pl.when(in_range(k))
            def _():
                last_hop(k).wait()
                dhf[:, cols] = fk[...] + r3[k % 2]

            k2 = s - 2

            @pl.when(in_range(k2))
            def _():
                z_wait(zc(k2, 2), 2)
                sl, zs = k2 % 3, k2 % 2
                fs[...] = r1[sl, z, 1 - q]
                fk[...] = r1[sl, z, q]
                for cond, buf in ((z >= 1, zr), (z <= 2, zl)):
                    @pl.when(cond)
                    def _(buf=buf):
                        fs[...] += buf[2, zs, 1 - q]
                        fk[...] += buf[2, zs, q]

                last_hop(k2).start()

            k1 = s - 1

            @pl.when(in_range(k1))
            def _():
                first(k1).wait()
                for b in range(4):
                    kept = op[k1 % 2, b, :, x, :, cols] if axis == "x" else op[k1 % 2, b, y, :, :, cols]
                    r1[k1 % 3, b] += kept
                z_start(zc(k1, 0), zr, zl, r1, k1 % 3, 0, k1 % 2)

        def move(s, t):
            k = s - 2

            @pl.when(in_range(k))
            def _():
                z_wait(zc(k, t - 1), t - 1)
                z_start(zc(k, t), zr, zl, r1, k % 3, t, k % 2)

        return open_up, turn, move

    def three_axes():
        cols = pl.ds(COL_A + COL_B, COL_C)

        def first(k):
            return hop(op.at[k % 2, :, :, 1 - x, :, cols], r1c.at[k % 3], sem_c["first"], k, nbr_x)

        def second(k):
            return hop(r1c.at[k % 3, :, 1 - y], r2c.at[k % 3], sem_c["last"], k, nbr_y)

        def zc(k, t):
            return z_copies(zrc, zlc, r2c, k % 3, t, k % 2, sem_c["z"], k % 2)

        def open_up(s):
            @pl.when(in_range(s))
            def _():
                first(s).start()

        def turn(s):
            k = s - 3

            @pl.when(in_range(k))
            def _():
                z_wait(zc(k, 2), 2)
                dhf[:, cols] = r2c[k % 3, z]
                for cond, buf in ((z >= 1, zrc), (z <= 2, zlc)):
                    @pl.when(cond)
                    def _(buf=buf):
                        dhf[:, cols] += buf[2, k % 2]

            k2 = s - 2

            @pl.when(in_range(k2))
            def _():
                second(k2).wait()
                for b in range(4):
                    r2c[k2 % 3, b] += r1c[k2 % 3, b, y]
                z_start(zc(k2, 0), zrc, zlc, r2c, k2 % 3, 0, k2 % 2)

            k1 = s - 1

            @pl.when(in_range(k1))
            def _():
                first(k1).wait()
                for b in range(4):
                    r1c[k1 % 3, b] += op[k1 % 2, b, :, x, :, cols]
                second(k1).start()

        def move(s, t):
            k = s - 3

            @pl.when(in_range(k))
            def _():
                z_wait(zc(k, t - 1), t - 1)
                z_start(zc(k, t), zrc, zlc, r2c, k % 3, t, k % 2)

        return open_up, turn, move

    open_a, turn_a, move_a = two_axes("x", 0, COL_A, r1a, zra, zla, fsa, fka, r3a, sem_a)
    open_b, turn_b, move_b = two_axes("y", COL_A, COL_B, r1b, zrb, zlb, fsb, fkb, r3b, sem_b)
    open_c, turn_c, move_c = three_axes()

    def finish(k):
        load_own(k).wait()

        @pl.when(k >= 2)
        def _():
            store_dx(k - 2).wait()

        xo = xr[k % 2].astype(jnp.float32)
        inv = lax.rsqrt(jnp.mean(xo * xo, axis=-1, keepdims=True) + NORM_EPS)
        xh = xo * inv
        dh = dhf[...] / LOGIT_SCALE
        dgacc[...] += dh * xh
        u = dh * gain[...]
        dxb[k % 2] = inv * (u - xh * jnp.mean(u * xh, axis=-1, keepdims=True))
        store_dx(k).start()

    def tell_neighbours():
        pl.semaphore_signal(nbr.at[0], 1, device_id=nbr_x, device_id_type=MESH)
        pl.semaphore_signal(nbr.at[1], 1, device_id=nbr_y, device_id_type=MESH)

        @pl.when(z <= 2)
        def _():
            pl.semaphore_signal(nbr.at[2], 1, device_id=nbr_r, device_id_type=MESH)

        @pl.when(z >= 1)
        def _():
            pl.semaphore_signal(nbr.at[3], 1, device_id=nbr_l, device_id_type=MESH)

    def hear_neighbours():
        pl.semaphore_wait(nbr.at[0], 1)
        pl.semaphore_wait(nbr.at[1], 1)

        @pl.when(z >= 1)
        def _():
            pl.semaphore_wait(nbr.at[2], 1)

        @pl.when(z <= 2)
        def _():
            pl.semaphore_wait(nbr.at[3], 1)

    with jax.named_scope("init"):
        for half in range(2):
            load_x(0, half).start()
        for j in range(len(blocks)):
            tab_block(j).start()
        barrier = pltpu.get_barrier_semaphore()
        for q in range(1, 32):
            pl.semaphore_signal(barrier, 1, device_id=peer(q), device_id_type=MESH)
        tacc[...] = jnp.zeros_like(tacc)
        tacc[2:3, :] = jnp.broadcast_to(jnp.sum(tok[1], keepdims=True), (1, ROWS))
        dgacc[...] = jnp.zeros_like(dgacc)
    with jax.named_scope("norm0"):
        for half in range(2):
            load_x(0, half).wait()
        norm(0)
        for half in range(2):
            load_x(1, half).start()
        for j in range(len(blocks)):
            tab_block(j).wait()

    last = n_chunks + DEPTH

    def iteration(i, _):
        s = i - 1
        busy = in_range(s)
        ahead = i < n_chunks
        scope = jax.named_scope

        with scope("logits"):
            @pl.when(ahead)
            def _():
                top = logits(i)
                st[i % 2, 0] = local_lse(i, top)

        with scope("tell"):
            @pl.when(i == 0)
            def _():
                pl.semaphore_wait(barrier, 31)

            @pl.when(ahead)
            def _():
                start(swap32(st, i % 2, sem_st))

        with scope("b0"):
            turn_b(s)

        with scope("partner"):
            @pl.when(busy)
            def _():
                add_partner(s)

            open_a(s)
            open_b(s)
            open_c(s)

            @pl.when(in_range(s - 3))
            def _():
                load_own(s - 3).start()

        with scope("zero"):
            @pl.when(i == 0)
            def _():
                acc[...] = jnp.zeros_like(acc)

        with scope("de0"):
            @pl.when(busy)
            def _():
                embed_grad(s, 0)

        with scope("ac0"):
            turn_a(s)
            turn_c(s)

            @pl.when((i >= 1) & (i < last))
            def _():
                tell_neighbours()

        with scope("finish"):
            @pl.when(in_range(s - 3))
            def _():
                finish(s - 3)

        with scope("de1"):
            @pl.when(busy)
            def _():
                embed_grad(s, 1)

            @pl.when(i == n_chunks)
            def _():
                pltpu.make_async_copy(acc, de_out, sem_out.at[2]).start()

        with scope("hear"):
            @pl.when((i >= 1) & (i < last))
            def _():
                hear_neighbours()

        with scope("b1"):
            move_b(i, 1)

        with scope("norm"):
            @pl.when(i + 1 < n_chunks)
            def _():
                for half in range(2):
                    load_x(i + 1, half).wait()
                norm(i + 1)

            @pl.when(i + 2 < n_chunks)
            def _():
                for half in range(2):
                    load_x(i + 2, half).start()

        with scope("stat"):
            @pl.when(ahead)
            def _():
                wait(swap32(st, i % 2, sem_st))

        with scope("dz"):
            @pl.when(ahead)
            def _():
                lse = merge(st, i % 2, 32)
                tacc[0:1, :] += weights(i) * lse
                grad_logits(i, lse)

        with scope("ac1"):
            move_a(i, 1)
            move_c(i, 1)

        with scope("dh0"):
            @pl.when(ahead)
            def _():
                hidden_grad(i, 0)

        with scope("b2"):
            move_b(i, 2)

        with scope("dh1"):
            @pl.when(ahead)
            def _():
                hidden_grad(i, 1)

        with scope("ac2"):
            move_a(i, 2)
            move_c(i, 2)

        return 0

    lax.fori_loop(0, last + 1, iteration, 0)
    with jax.named_scope("gain"):
        dg1[0, 0, :, 0:width] = jnp.sum(dgacc[...], axis=0, keepdims=True)
        dg1[0, 0, :, width : width + ROWS] = tacc[1:2, :]
        start(swap8(dg1, 0, sem_g1))
        wait(swap8(dg1, 0, sem_g1))
        dg2[0, 0] = sum(dg1[0, q] for q in range(8))
        start(swap4(dg2, 0, sem_g2))
        wait(swap4(dg2, 0, sem_g2))
        total = sum(dg2[0, q] for q in range(4))
        sums_out[:, 0:width] = total[:, 0:width]
        sums_out[:, width : width + ROWS] = tacc[0:1, :] - total[:, width : width + ROWS]
        for n in (n_chunks - 2, n_chunks - 1):
            store_dx(n).wait()
        pltpu.make_async_copy(acc, de_out, sem_out.at[2]).wait()


def hand_over_kernel(de_in, dx_in, sums_in, de_out, dx_out, dg_out, loss_out, buf, sem):
    step = buf.shape[1]
    gets, puts = [], []
    for src, dst in ((de_in, de_out), (dx_in, dx_out)):
        rows = src.shape[0]
        for r in range(0, rows, step):
            n, some = len(gets), pl.ds(r, min(step, rows - r))
            here = buf.at[n, pl.ds(0, some.size)]
            gets.append(pltpu.make_async_copy(src.at[some], here, sem.at[0, n]))
            puts.append(pltpu.make_async_copy(here, dst.at[some], sem.at[1, n]))
    for get in gets:
        get.start()
    width = de_in.shape[1]
    dg_out[...] = sums_in[:, 0:width]
    loss_out[...] = jnp.sum(sums_in[:, width : width + ROWS], keepdims=True)
    for get in gets:
        get.wait()
    scaled = de_in.shape[0]
    for n, put in enumerate(puts):
        if n * step < scaled:
            buf[n] = buf[n] * (1.0 / LOGIT_SCALE)
        put.start()
    for put in puts:
        put.wait()


def solution(mesh):
    def local_step(residual, labels, loss_mask, norm_gain, table_shard):
        tokens, width = residual.shape
        vocab = table_shard.shape[0]
        n_chunks = tokens // ROWS
        f32, bf16 = jnp.float32, jnp.bfloat16

        tok = jnp.stack([labels.astype(f32), loss_mask]).reshape(2, 16, 2, n_chunks, GROUP)
        tok = tok.transpose(0, 3, 2, 1, 4).reshape(2, n_chunks, ROWS)
        dma = pltpu.SemaphoreType.DMA
        vm = pltpu.VMEM
        slab = (GROUP, width)
        pair, ways = (2, 2), (2, 2, 3, 2)
        scratch = [vm((vocab, width), bf16), vm((3, 32, *slab), bf16), vm((vocab, ROWS), f32)]
        scratch += [vm((vocab, ROWS), bf16), vm((ROWS, vocab), bf16), vm((vocab, width), f32)]
        scratch += [vm((3, *GRID, *slab), f32), vm((*GRID, *slab), f32)]
        scratch += [vm((3, 4, 2, GROUP, n), f32) for n in (COL_A, COL_B)]
        scratch += [vm((3, 4, 2, GROUP, COL_C), f32), vm((3, 4, GROUP, COL_C), f32)]
        for n in (COL_A, COL_B):
            scratch += [vm((3, 2, 2, GROUP, n), f32)] * 2
        scratch += [vm((3, 2, GROUP, COL_C), f32)] * 2
        for n in (COL_A, COL_B):
            scratch += [vm((GROUP, n), f32), vm((GROUP, n), f32), vm((2, GROUP, n), f32)]
        scratch += [vm((2, 32, 1, ROWS), f32), vm((GROUP, ROWS), f32), vm((32, GROUP, 128), f32)]
        scratch += [vm(slab, f32), vm((2, *slab), bf16), vm((2, *slab), f32), vm(slab, f32)]
        scratch += [vm((1, n, 1, width + ROWS), f32) for n in (8, 4)]
        scratch += [dma((4,)), dma((8,)), dma((3,)), dma(pair), pltpu.SemaphoreType.REGULAR, pltpu.SemaphoreType.REGULAR((4,))]
        scratch += [dma((2, 2, 32)), dma((2, 1, 8)), dma((2, 1, 4))]
        scratch += [{"first": dma(pair), "z": dma(ways), "last": dma(pair)}] * 3
        whole = pl.BlockSpec(memory_space=pltpu.VMEM)
        raw = pl.BlockSpec(memory_space=pl.ANY)
        dx, de, sums = pl.pallas_call(
            functools.partial(step_kernel, n_chunks),
            out_shape=(
                jax.ShapeDtypeStruct((n_chunks, GROUP, width), f32),
                jax.ShapeDtypeStruct((vocab, width), f32),
                jax.ShapeDtypeStruct((1, width + ROWS), f32),
            ),
            in_specs=[raw, whole, whole, raw],
            out_specs=(raw, raw, whole),
            scratch_shapes=scratch,
            compiler_params=pltpu.CompilerParams(vmem_limit_bytes=VMEM_LIMIT, has_side_effects=True, collective_id=0),
            name="head_step",
        )(
            residual.reshape(16, 2, n_chunks, GROUP, width),
            tok,
            norm_gain.reshape(1, width),
            table_shard,
        )
        de, dx, dg, loss = pl.pallas_call(
            hand_over_kernel,
            out_shape=(
                jax.ShapeDtypeStruct((vocab, width), f32),
                jax.ShapeDtypeStruct((n_chunks * GROUP, width), f32),
                jax.ShapeDtypeStruct((1, width), f32),
                jax.ShapeDtypeStruct((1, 1), f32),
            ),
            in_specs=[raw, raw, whole],
            out_specs=(raw, raw, whole, whole),
            scratch_shapes=[vm((16, 128, width), f32), dma((2, 16))],
            compiler_params=pltpu.CompilerParams(vmem_limit_bytes=VMEM_LIMIT),
            name="hand_over",
        )(de, dx.reshape(n_chunks * GROUP, width), sums)
        return loss.reshape(()), dx, de, dg.reshape(width)

    return jax.shard_map(local_step, mesh=mesh, in_specs=(P(), P(), P(), P(), P("vp", None)), out_specs=(P(), P("vp", None), P("vp", None), P()), check_vma=False)
```

```python
import functools

import jax
import jax.numpy as jnp
from jax import lax
from jax.experimental import pallas as pl
from jax.experimental.pallas import tpu as pltpu
from jax.sharding import PartitionSpec as P

VOCAB_REAL = 49155
LOGIT_SCALE = 6.0
NORM_EPS = 1e-6
INV_SCALE = 1.0 / LOGIT_SCALE
MESH = pl.DeviceIdType.MESH

GROUP = 8
ROWS = 32 * GROUP
COL_A, COL_B, COL_C = 896, 1792, 1408
DEPTH = 3
VMEM_LIMIT = 67043328
GRID = (4, 2, 2)


def step_kernel(
    n_chunks, res, tok, gain, tab,
    dx_out, de_out, sums_out,
    ev, h, zt, dzt, dz, acc, op, r0,
    r1a, r1b, r1c, r2c, zra, zla, zrb, zlb, zrc, zlc,
    fsa, fka, r3a, fsb, fkb, r3b,
    st, tacc, ssq, dhf, xr, dxb, dgacc, dg1, dg2,
    sem_in, sem_tab, sem_out, sem_p, cred, nbr, sem_st, sem_g1, sem_g2,
    sem_a, sem_b, sem_c,
):
    vocab, width = ev.shape
    edges = list(range(0, max(vocab - 511, 1), 512)) + [vocab]
    blocks = [(a, b - a) for a, b in zip(edges, edges[1:])]
    me = lax.axis_index("vp")
    c, x, y, z = me % 2, (me // 2) % 2, (me // 4) % 2, me // 8

    def dev(zz, yy, xx, cc):
        return (((zz * 2 + yy) * 2 + xx) * 2 + cc,)

    def send(src, dst, ssem, rsem, to):
        return pltpu.make_async_remote_copy(src, dst, ssem, rsem, device_id=to, device_id_type=MESH)

    def hop(src, dst, sem, k, to):
        return send(src, dst, sem.at[0, k % 2], sem.at[1, k % 2], to)

    nbr_x, nbr_y = dev(z, y, 1 - x, c), dev(z, 1 - y, x, c)
    nbr_r, nbr_l = dev(z + 1, y, x, c), dev(z - 1, y, x, c)
    partner = dev(z, y, x, 1 - c)

    def load_x(n, half):
        return pltpu.make_async_copy(res.at[:, half, n], h.at[n % 3, pl.ds(16 * half, 16)], sem_in.at[half])

    def tab_block(j):
        a, m = blocks[j]
        return pltpu.make_async_copy(tab.at[pl.ds(a, m)], ev.at[pl.ds(a, m)], sem_tab.at[j])

    def load_own(n):
        return pltpu.make_async_copy(res.at[me // 2, me % 2, n], xr.at[n % 2], sem_in.at[2 + n % 2])

    def store_dx(n):
        return pltpu.make_async_copy(dxb.at[n % 2], dx_out.at[n], sem_out.at[n % 2])

    def label_rows(n):
        return tok[0, pl.ds(n, 1), :].astype(jnp.int32) - me * vocab

    def weights(n):
        return tok[1, pl.ds(n, 1), :] / tacc[2:3, :]

    def norm(n):
        slot = n % 3
        pieces = range(0, width, 256)

        def piece(i, j):
            return h[slot, i, :, j : j + 256].astype(jnp.float32)

        def squares(i, _):
            sums = [None] * 4
            for n_piece, j in enumerate(pieces):
                sq = piece(i, j)
                sq = sq * sq
                for b in range(2):
                    part, to = sq[:, 128 * b : 128 * (b + 1)], 2 * (n_piece % 2) + b
                    sums[to] = part if sums[to] is None else sums[to] + part
            ssq[i] = (sums[0] + sums[1]) + (sums[2] + sums[3])
            return 0

        def scale(i, _):
            inv = jnp.concatenate([ssq[i], ssq[i]], axis=1)
            for j in pieces:
                h[slot, i, :, j : j + 256] = ((piece(i, j) * inv) * gain[:, j : j + 256]).astype(jnp.bfloat16)
            return 0

        lax.fori_loop(0, 32, squares, 0, unroll=4)
        mean = jnp.sum(ssq[...], axis=-1, keepdims=True) * (1.0 / width)
        ssq[...] = jnp.broadcast_to(lax.rsqrt(mean + NORM_EPS), ssq.shape)
        lax.fori_loop(0, 32, scale, 0, unroll=4)

    def logits(n):
        top = jnp.full((1, ROWS), -jnp.inf, jnp.float32)
        hn = h[n % 3].reshape(ROWS, width)
        for a, m in blocks:
            t = lax.dot_general(ev[a : a + m, :], hn, (((1,), (1,)), ((), ())), preferred_element_type=jnp.float32)
            t = t * INV_SCALE
            ids = me * vocab + a + lax.broadcasted_iota(jnp.int32, (m, ROWS), 0)
            t = jnp.where(ids < VOCAB_REAL, t, -jnp.inf)
            zt[a : a + m, :] = t
            top = jnp.maximum(top, jnp.max(t, axis=0, keepdims=True))
        return top

    full_tiles = vocab // 128
    tail = vocab - full_tiles * 128

    def local_lse(n, top):
        lb = label_rows(n)

        def part(a, m, s, t):
            v = zt[pl.ds(a, m), :]
            ids = a + lax.broadcasted_iota(jnp.int32, (m, ROWS), 0)
            e = jnp.exp(v - top).reshape(m // 8, 8, ROWS)
            hit = jnp.where(ids == lb, v, 0.0).reshape(m // 8, 8, ROWS)
            return s + jnp.sum(e, axis=0), t + jnp.sum(hit, axis=0)

        zero = jnp.zeros((8, ROWS), jnp.float32)
        s, t = lax.fori_loop(0, full_tiles, lambda i, v: part(pl.multiple_of(i * 128, 128), 128, *v), (zero, zero), unroll=4)
        s, t = part(full_tiles * 128, tail, s, t)
        tacc[1:2, :] += weights(n) * jnp.sum(t, axis=0, keepdims=True)
        return top + jnp.log(jnp.sum(s, axis=0, keepdims=True))

    def merge(ref, slot, count):
        rows = [ref[slot, q] for q in range(count)]
        top = functools.reduce(jnp.maximum, rows)
        return top + jnp.log(sum(jnp.exp(r - top) for r in rows))

    def grad_logits(k, lse):
        lb = label_rows(k)
        w = weights(k)
        for a, m in [(i * 128, 128) for i in range(full_tiles)] + [(full_tiles * 128, tail)]:
            ids = a + lax.broadcasted_iota(jnp.int32, (m, ROWS), 0)
            p = jnp.exp(zt[a : a + m, :] - lse)
            d = (jnp.where(ids == lb, p - 1.0, p) * w).astype(jnp.bfloat16)
            dzt[a : a + m, :] = d
            dz[:, a : a + m] = d.T

    def embed_grad(k, half):
        tile = width // 4
        for a, m in blocks:
            for j in (2 * half, 2 * half + 1):
                cols = pl.ds(j * tile, tile)
                acc[a : a + m, cols] += jnp.dot(dzt[a : a + m, :], h[k % 3, :, :, cols].reshape(ROWS, tile), preferred_element_type=jnp.float32)

    split = width * 3 // 4
    parts = (pl.ds(0, split), pl.ds(split, width - split))

    def send_p(part):
        cols = parts[part]
        return send(op.at[2, :, :, :, :, cols], r0.at[:, :, :, :, cols], sem_p.at[0, part], sem_p.at[1, part], partner)

    def hidden_grad(k, part):
        own = k % 2
        where = ((1 - c) * own + c * 2, c * own + (1 - c) * 2)
        cols = parts[part]
        r = jnp.dot(dz[...], ev[:, cols], preferred_element_type=jnp.float32)
        for q in range(2):
            op[where[q], :, :, :, :, cols] = r[q * 128 : (q + 1) * 128].reshape(4, 2, 2, 8, cols.size)
        if part == 0:
            @pl.when(k >= 1)
            def _():
                pl.semaphore_wait(cred, 1)
        send_p(part).start()

    def add_partner(k):
        for half in range(2):
            send_p(half).wait()

        def body(i, _):
            op[k % 2, i] += r0[i]
            return 0

        lax.fori_loop(0, 4, body, 0)

        @pl.when(k < n_chunks - 1)
        def _():
            pl.semaphore_signal(cred, 1, device_id=partner, device_id_type=MESH)

    def peer(q):
        qy, qx, qc = (q // 4) % 2, (q // 2) % 2, q % 2
        return dev((z + q // 8) % 4, y + qy * (1 - 2 * y), x + qx * (1 - 2 * x), c + qc * (1 - 2 * c))

    def swap8(buf, slot, sem):
        return [send(buf.at[slot, 0], buf.at[slot, q], sem.at[0, slot, q], sem.at[1, slot, q], peer(q)) for q in range(1, 8)]

    def swap32(buf, slot, sem):
        out = []
        for q in range(1, 32):
            there = ((4 - q // 8) % 4) * 8 + q % 8
            out.append(send(buf.at[slot, 0], buf.at[slot, there], sem.at[0, slot, q], sem.at[1, slot, there], peer(q)))
        return out

    def swap4(buf, slot, sem):
        return [
            send(buf.at[slot, 0], buf.at[slot, 4 - q], sem.at[0, slot, q], sem.at[1, slot, 4 - q], peer(8 * q))
            for q in range(1, 4)
        ]

    def start(copies):
        for cp in copies:
            cp.start()

    def wait(copies):
        for cp in copies:
            cp.wait_send()
        for cp in copies:
            cp.wait_recv()

    def z_copies(zr, zl, s1, sl, t, zslot, sem, par):
        ways = []
        for way, (buf, to, block) in enumerate(((zr, nbr_r, 3 - t), (zl, nbr_l, t))):
            sems = (sem.at[0, way, t, par], sem.at[1, way, t, par])
            first = send(s1.at[sl, block], buf.at[t, zslot], *sems, to)
            later = send(buf.at[t - 1, zslot], buf.at[t, zslot], *sems, to) if t else None
            behind, ahead = (z, 3 - z) if way == 0 else (3 - z, z)
            ways.append((behind, ahead, first, later))
        return ways

    def z_wait(ways, t):
        for behind, ahead, first, _ in ways:
            @pl.when((behind <= t) & (ahead > 0))
            def _(first=first):
                first.wait_send()

            @pl.when((behind > 0) & (behind <= t + 1))
            def _(first=first):
                first.wait_recv()

    def z_start(ways, zr, zl, s1, sl, t, zslot):
        for (behind, ahead, first, later), buf, block in zip(ways, (zr, zl), (3 - t + z, t - 3 + z)):
            @pl.when(behind == 0)
            def _(first=first):
                first.start()

            if t:
                @pl.when((behind > 0) & (behind <= t) & (ahead > 0))
                def _(buf=buf, block=block, later=later):
                    buf[t - 1, zslot] += s1[sl, block]
                    later.start()

    def in_range(k):
        return (k >= 0) & (k < n_chunks)

    def two_axes(axis, col, size, r1, zr, zl, fs, fk, r3, sem):
        cols = pl.ds(col, size)
        first_nbr, last_nbr = (nbr_x, nbr_y) if axis == "x" else (nbr_y, nbr_x)
        q = y if axis == "x" else x

        def first(k):
            src = op.at[k % 2, :, :, 1 - x, :, cols] if axis == "x" else op.at[k % 2, :, 1 - y, :, :, cols]
            return hop(src, r1.at[k % 3], sem["first"], k, first_nbr)

        def last_hop(k):
            return hop(fs, r3.at[k % 2], sem["last"], k, last_nbr)

        def zc(k, t):
            return z_copies(zr, zl, r1, k % 3, t, k % 2, sem["z"], k % 2)

        def open_up(s):
            @pl.when(in_range(s))
            def _():
                first(s).start()

        def turn(s):
            k = s - 3

            @pl.when(in_range(k))
            def _():
                last_hop(k).wait()
                dhf[:, cols] = fk[...] + r3[k % 2]

            k2 = s - 2

            @pl.when(in_range(k2))
            def _():
                z_wait(zc(k2, 2), 2)
                sl, zs = k2 % 3, k2 % 2
                fs[...] = r1[sl, z, 1 - q]
                fk[...] = r1[sl, z, q]
                for cond, buf in ((z >= 1, zr), (z <= 2, zl)):
                    @pl.when(cond)
                    def _(buf=buf):
                        fs[...] += buf[2, zs, 1 - q]
                        fk[...] += buf[2, zs, q]

                last_hop(k2).start()

            k1 = s - 1

            @pl.when(in_range(k1))
            def _():
                first(k1).wait()
                for b in range(4):
                    kept = op[k1 % 2, b, :, x, :, cols] if axis == "x" else op[k1 % 2, b, y, :, :, cols]
                    r1[k1 % 3, b] += kept
                z_start(zc(k1, 0), zr, zl, r1, k1 % 3, 0, k1 % 2)

        def move(s, t):
            k = s - 2

            @pl.when(in_range(k))
            def _():
                z_wait(zc(k, t - 1), t - 1)
                z_start(zc(k, t), zr, zl, r1, k % 3, t, k % 2)

        return open_up, turn, move

    def three_axes():
        cols = pl.ds(COL_A + COL_B, COL_C)

        def first(k):
            return hop(op.at[k % 2, :, :, 1 - x, :, cols], r1c.at[k % 3], sem_c["first"], k, nbr_x)

        def second(k):
            return hop(r1c.at[k % 3, :, 1 - y], r2c.at[k % 3], sem_c["last"], k, nbr_y)

        def zc(k, t):
            return z_copies(zrc, zlc, r2c, k % 3, t, k % 2, sem_c["z"], k % 2)

        def open_up(s):
            @pl.when(in_range(s))
            def _():
                first(s).start()

        end = n_chunks - 1

        def to_z(k):
            second(k).wait()
            for b in range(4):
                r2c[k % 3, b] += r1c[k % 3, b, y]
            z_start(zc(k, 0), zrc, zlc, r2c, k % 3, 0, k % 2)

        def along_z(k, t):
            z_wait(zc(k, t - 1), t - 1)
            z_start(zc(k, t), zrc, zlc, r2c, k % 3, t, k % 2)

        def off_z(k):
            z_wait(zc(k, 2), 2)
            dhf[:, cols] = r2c[k % 3, z]
            for cond, buf in ((z >= 1, zrc), (z <= 2, zlc)):
                @pl.when(cond)
                def _(buf=buf):
                    dhf[:, cols] += buf[2, k % 2]

        def turn(s):
            @pl.when(in_range(s - 3) & (s - 3 != end))
            def _():
                off_z(s - 3)

            @pl.when(in_range(s - 2) & (s - 2 != end))
            def _():
                to_z(s - 2)

            @pl.when(s - 2 == end)
            def _():
                along_z(end, 1)

            k1 = s - 1

            @pl.when(in_range(k1))
            def _():
                first(k1).wait()
                for b in range(4):
                    r1c[k1 % 3, b] += op[k1 % 2, b, :, x, :, cols]
                second(k1).start()

        def move(s, t):
            @pl.when(in_range(s - 3) & (s - 3 != end))
            def _():
                along_z(s - 3, t)

            if t == 1:
                @pl.when(s - 3 == end)
                def _():
                    along_z(end, 2)
            else:
                @pl.when(s - 2 == end)
                def _():
                    to_z(end)

                @pl.when(s - 3 == end)
                def _():
                    off_z(end)

        return open_up, turn, move

    open_a, turn_a, move_a = two_axes("x", 0, COL_A, r1a, zra, zla, fsa, fka, r3a, sem_a)
    open_b, turn_b, move_b = two_axes("y", COL_A, COL_B, r1b, zrb, zlb, fsb, fkb, r3b, sem_b)
    open_c, turn_c, move_c = three_axes()

    def finish(k):
        load_own(k).wait()

        @pl.when(k >= 2)
        def _():
            store_dx(k - 2).wait()

        xo = xr[k % 2].astype(jnp.float32)
        dh = dhf[...] * INV_SCALE
        u = dh * gain[...]
        inv = lax.rsqrt(jnp.mean(xo * xo, axis=-1, keepdims=True) + NORM_EPS)
        slope = inv * jnp.mean(u * xo, axis=-1, keepdims=True)
        xh = xo * inv
        dgacc[...] += dh * xh
        dxb[k % 2] = inv * (u - xh * slope)
        store_dx(k).start()

    def tell_neighbours():
        pl.semaphore_signal(nbr.at[0], 1, device_id=nbr_x, device_id_type=MESH)
        pl.semaphore_signal(nbr.at[1], 1, device_id=nbr_y, device_id_type=MESH)

        @pl.when(z <= 2)
        def _():
            pl.semaphore_signal(nbr.at[2], 1, device_id=nbr_r, device_id_type=MESH)

        @pl.when(z >= 1)
        def _():
            pl.semaphore_signal(nbr.at[3], 1, device_id=nbr_l, device_id_type=MESH)

    def hear_neighbours():
        pl.semaphore_wait(nbr.at[0], 1)
        pl.semaphore_wait(nbr.at[1], 1)

        @pl.when(z >= 1)
        def _():
            pl.semaphore_wait(nbr.at[2], 1)

        @pl.when(z <= 2)
        def _():
            pl.semaphore_wait(nbr.at[3], 1)

    with jax.named_scope("init"):
        for half in range(2):
            load_x(0, half).start()
        for j in range(len(blocks)):
            tab_block(j).start()
        barrier = pltpu.get_barrier_semaphore()
        for q in range(1, 32):
            pl.semaphore_signal(barrier, 1, device_id=peer(q), device_id_type=MESH)
        tacc[...] = jnp.zeros_like(tacc)
        tacc[2:3, :] = jnp.broadcast_to(jnp.sum(tok[1], keepdims=True), (1, ROWS))
        dgacc[...] = jnp.zeros_like(dgacc)
    with jax.named_scope("norm0"):
        for half in range(2):
            load_x(0, half).wait()
        norm(0)
        for half in range(2):
            load_x(1, half).start()
        for j in range(len(blocks)):
            tab_block(j).wait()

    last = n_chunks + DEPTH

    def iteration(i, _):
        s = i - 1
        busy = in_range(s)
        ahead = i < n_chunks
        scope = jax.named_scope

        with scope("logits"):
            @pl.when(ahead)
            def _():
                top = logits(i)
                st[i % 2, 0] = local_lse(i, top)

        with scope("tell"):
            @pl.when(i == 0)
            def _():
                pl.semaphore_wait(barrier, 31)

            @pl.when(ahead)
            def _():
                start(swap32(st, i % 2, sem_st))

        with scope("b0"):
            turn_b(s)

        with scope("partner"):
            @pl.when(busy)
            def _():
                add_partner(s)

            open_a(s)
            open_b(s)
            open_c(s)

        with scope("zero"):
            @pl.when(i == 0)
            def _():
                acc[...] = jnp.zeros_like(acc)

        with scope("de0"):
            @pl.when(busy)
            def _():
                embed_grad(s, 0)

        with scope("ac0"):
            turn_a(s)
            turn_c(s)

            @pl.when((i >= 1) & (i < last))
            def _():
                tell_neighbours()

        with scope("finish"):
            @pl.when(in_range(s - 3))
            def _():
                finish(s - 3)

            @pl.when(in_range(s - 2))
            def _():
                load_own(s - 2).start()

        with scope("de1"):
            @pl.when(busy)
            def _():
                embed_grad(s, 1)

            @pl.when(i == n_chunks)
            def _():
                pltpu.make_async_copy(acc, de_out, sem_out.at[2]).start()

        with scope("hear"):
            @pl.when((i >= 1) & (i < last))
            def _():
                hear_neighbours()

        with scope("b1"):
            move_b(i, 1)

        with scope("norm"):
            @pl.when(i + 1 < n_chunks)
            def _():
                for half in range(2):
                    load_x(i + 1, half).wait()
                norm(i + 1)

            @pl.when(i + 2 < n_chunks)
            def _():
                for half in range(2):
                    load_x(i + 2, half).start()

        with scope("stat"):
            @pl.when(ahead)
            def _():
                wait(swap32(st, i % 2, sem_st))

        with scope("dz"):
            @pl.when(ahead)
            def _():
                lse = merge(st, i % 2, 32)
                tacc[0:1, :] += weights(i) * lse
                grad_logits(i, lse)

        with scope("ac1"):
            move_a(i, 1)
            move_c(i, 1)

        with scope("dh0"):
            @pl.when(ahead)
            def _():
                hidden_grad(i, 0)

        with scope("b2"):
            move_b(i, 2)

        with scope("dh1"):
            @pl.when(ahead)
            def _():
                hidden_grad(i, 1)

        with scope("ac2"):
            move_a(i, 2)
            move_c(i, 2)

        return 0

    lax.fori_loop(0, last + 1, iteration, 0)
    with jax.named_scope("gain"):
        dg1[0, 0, :, 0:width] = jnp.sum(dgacc[...], axis=0, keepdims=True)
        dg1[0, 0, :, width : width + ROWS] = tacc[1:2, :]
        start(swap8(dg1, 0, sem_g1))
        wait(swap8(dg1, 0, sem_g1))
        dg2[0, 0] = sum(dg1[0, q] for q in range(8))
        start(swap4(dg2, 0, sem_g2))
        wait(swap4(dg2, 0, sem_g2))
        total = sum(dg2[0, q] for q in range(4))
        sums_out[:, 0:width] = total[:, 0:width]
        sums_out[:, width : width + ROWS] = tacc[0:1, :] - total[:, width : width + ROWS]
        for n in (n_chunks - 2, n_chunks - 1):
            store_dx(n).wait()
        pltpu.make_async_copy(acc, de_out, sem_out.at[2]).wait()


def hand_over_kernel(de_in, dx_in, sums_in, de_out, dx_out, dg_out, loss_out, buf, sem):
    step = buf.shape[1]
    gets, puts = [], []
    for src, dst in ((de_in, de_out), (dx_in, dx_out)):
        rows = src.shape[0]
        for r in range(0, rows, step):
            n, some = len(gets), pl.ds(r, min(step, rows - r))
            here = buf.at[n, pl.ds(0, some.size)]
            gets.append(pltpu.make_async_copy(src.at[some], here, sem.at[0, n]))
            puts.append(pltpu.make_async_copy(here, dst.at[some], sem.at[1, n]))
    for get in gets:
        get.start()
    width = de_in.shape[1]
    dg_out[...] = sums_in[:, 0:width]
    loss_out[...] = jnp.sum(sums_in[:, width : width + ROWS], keepdims=True)
    for get in gets:
        get.wait()
    scaled = de_in.shape[0]
    for n, put in enumerate(puts):
        if n * step < scaled:
            buf[n] = buf[n] * INV_SCALE
        put.start()
    for put in puts:
        put.wait()


def solution(mesh):
    def local_step(residual, labels, loss_mask, norm_gain, table_shard):
        tokens, width = residual.shape
        vocab = table_shard.shape[0]
        n_chunks = tokens // ROWS
        f32, bf16 = jnp.float32, jnp.bfloat16

        tok = jnp.stack([labels.astype(f32), loss_mask]).reshape(2, 16, 2, n_chunks, GROUP)
        tok = tok.transpose(0, 3, 2, 1, 4).reshape(2, n_chunks, ROWS)
        dma = pltpu.SemaphoreType.DMA
        vm = pltpu.VMEM
        slab = (GROUP, width)
        pair, ways = (2, 2), (2, 2, 3, 2)
        scratch = [vm((vocab, width), bf16), vm((3, 32, *slab), bf16), vm((vocab, ROWS), f32)]
        scratch += [vm((vocab, ROWS), bf16), vm((ROWS, vocab), bf16), vm((vocab, width), f32)]
        scratch += [vm((3, *GRID, *slab), f32), vm((*GRID, *slab), f32)]
        scratch += [vm((3, 4, 2, GROUP, n), f32) for n in (COL_A, COL_B)]
        scratch += [vm((3, 4, 2, GROUP, COL_C), f32), vm((3, 4, GROUP, COL_C), f32)]
        for n in (COL_A, COL_B):
            scratch += [vm((3, 2, 2, GROUP, n), f32)] * 2
        scratch += [vm((3, 2, GROUP, COL_C), f32)] * 2
        for n in (COL_A, COL_B):
            scratch += [vm((GROUP, n), f32), vm((GROUP, n), f32), vm((2, GROUP, n), f32)]
        scratch += [vm((2, 32, 1, ROWS), f32), vm((GROUP, ROWS), f32), vm((32, GROUP, 128), f32)]
        scratch += [vm(slab, f32), vm((2, *slab), bf16), vm((2, *slab), f32), vm(slab, f32)]
        scratch += [vm((1, n, 1, width + ROWS), f32) for n in (8, 4)]
        scratch += [dma((4,)), dma((8,)), dma((3,)), dma(pair), pltpu.SemaphoreType.REGULAR, pltpu.SemaphoreType.REGULAR((4,))]
        scratch += [dma((2, 2, 32)), dma((2, 1, 8)), dma((2, 1, 4))]
        scratch += [{"first": dma(pair), "z": dma(ways), "last": dma(pair)}] * 3
        whole = pl.BlockSpec(memory_space=pltpu.VMEM)
        raw = pl.BlockSpec(memory_space=pl.ANY)
        dx, de, sums = pl.pallas_call(
            functools.partial(step_kernel, n_chunks),
            out_shape=(
                jax.ShapeDtypeStruct((n_chunks, GROUP, width), f32),
                jax.ShapeDtypeStruct((vocab, width), f32),
                jax.ShapeDtypeStruct((1, width + ROWS), f32),
            ),
            in_specs=[raw, whole, whole, raw],
            out_specs=(raw, raw, whole),
            scratch_shapes=scratch,
            compiler_params=pltpu.CompilerParams(vmem_limit_bytes=VMEM_LIMIT, has_side_effects=True, collective_id=0),
            name="head_step",
        )(
            residual.reshape(16, 2, n_chunks, GROUP, width),
            tok,
            norm_gain.reshape(1, width),
            table_shard,
        )
        de, dx, dg, loss = pl.pallas_call(
            hand_over_kernel,
            out_shape=(
                jax.ShapeDtypeStruct((vocab, width), f32),
                jax.ShapeDtypeStruct((n_chunks * GROUP, width), f32),
                jax.ShapeDtypeStruct((1, width), f32),
                jax.ShapeDtypeStruct((1, 1), f32),
            ),
            in_specs=[raw, raw, whole],
            out_specs=(raw, raw, whole, whole),
            scratch_shapes=[vm((16, 128, width), f32), dma((2, 16))],
            compiler_params=pltpu.CompilerParams(vmem_limit_bytes=VMEM_LIMIT),
            name="hand_over",
        )(de, dx.reshape(n_chunks * GROUP, width), sums)
        return loss.reshape(()), dx, de, dg.reshape(width)

    return jax.shard_map(local_step, mesh=mesh, in_specs=(P(), P(), P(), P(), P("vp", None)), out_specs=(P(), P("vp", None), P("vp", None), P()), check_vma=False)
```

```python
import functools

import jax
import jax.numpy as jnp
from jax import lax
from jax.experimental import pallas as pl
from jax.experimental.pallas import tpu as pltpu
from jax.sharding import PartitionSpec as P

VOCAB_REAL = 49155
LOGIT_SCALE = 6.0
NORM_EPS = 1e-6
INV_SCALE = 1.0 / LOGIT_SCALE
MESH = pl.DeviceIdType.MESH

GROUP = 8
ROWS = 32 * GROUP
COL_A, COL_B, COL_C = 896, 1792, 1408
DEPTH = 3
VMEM_LIMIT = 67043328
GRID = (4, 2, 2)


def step_kernel(
    n_chunks, res, tok, gain, tab,
    dx_out, de_out, sums_out,
    ev, h, zt, dzt, dz, acc, op, r0,
    r1a, r1b, r1c, r2c, zra, zla, zrb, zlb, zrc, zlc,
    fsa, fka, r3a, fsb, fkb, r3b,
    st, tacc, ssq, dhf, xr, dxb, dgacc, dg1, dg2,
    sem_in, sem_tab, sem_out, sem_p, cred, nbr, sem_st, sem_g1, sem_g2,
    sem_a, sem_b, sem_c,
):
    vocab, width = ev.shape
    edges = list(range(0, max(vocab - 511, 1), 512)) + [vocab]
    blocks = [(a, b - a) for a, b in zip(edges, edges[1:])]
    me = lax.axis_index("vp")
    c, x, y, z = me % 2, (me // 2) % 2, (me // 4) % 2, me // 8

    def dev(zz, yy, xx, cc):
        return (((zz * 2 + yy) * 2 + xx) * 2 + cc,)

    def par(k):
        return k % 2

    def send(src, dst, ssem, rsem, to):
        return pltpu.make_async_remote_copy(src, dst, ssem, rsem, device_id=to, device_id_type=MESH)

    def hop(src, dst, sem, k, to):
        return send(src, dst, sem.at[0, par(k)], sem.at[1, par(k)], to)

    nbr_x, nbr_y = dev(z, y, 1 - x, c), dev(z, 1 - y, x, c)
    nbr_r, nbr_l = dev(z + 1, y, x, c), dev(z - 1, y, x, c)
    partner = dev(z, y, x, 1 - c)

    def load_x(n, half):
        return pltpu.make_async_copy(res.at[:, half, n], h.at[n % 3, pl.ds(16 * half, 16)], sem_in.at[half])

    def tab_block(j):
        a, m = blocks[j]
        return pltpu.make_async_copy(tab.at[pl.ds(a, m)], ev.at[pl.ds(a, m)], sem_tab.at[j])

    def load_own(n):
        return pltpu.make_async_copy(res.at[me // 2, me % 2, n], xr.at[par(n)], sem_in.at[2 + par(n)])

    def store_dx(n):
        return pltpu.make_async_copy(dxb.at[par(n)], dx_out.at[n], sem_out.at[par(n)])

    def label_rows(n):
        return tok[0, pl.ds(n, 1), :].astype(jnp.int32) - me * vocab

    def weights(n):
        return tok[1, pl.ds(n, 1), :] / tacc[2:3, :]

    def norm(n):
        slot = n % 3
        pieces = range(0, width, 256)

        def piece(i, j):
            return h[slot, i, :, j : j + 256].astype(jnp.float32)

        def squares(i, _):
            sums = [None] * 4
            for n_piece, j in enumerate(pieces):
                sq = piece(i, j)
                sq = sq * sq
                for b in range(2):
                    part, to = sq[:, 128 * b : 128 * (b + 1)], 2 * (n_piece % 2) + b
                    sums[to] = part if sums[to] is None else sums[to] + part
            ssq[i] = (sums[0] + sums[1]) + (sums[2] + sums[3])
            return 0

        def scale(i, _):
            inv = jnp.concatenate([ssq[i], ssq[i]], axis=1)
            for j in pieces:
                h[slot, i, :, j : j + 256] = ((piece(i, j) * inv) * gain[:, j : j + 256]).astype(jnp.bfloat16)
            return 0

        lax.fori_loop(0, 32, squares, 0, unroll=4)
        mean = jnp.sum(ssq[...], axis=-1, keepdims=True) * (1.0 / width)
        ssq[...] = jnp.broadcast_to(lax.rsqrt(mean + NORM_EPS), ssq.shape)
        lax.fori_loop(0, 32, scale, 0, unroll=4)

    def logits(n):
        top = jnp.full((1, ROWS), -jnp.inf, jnp.float32)
        hn = h[n % 3].reshape(ROWS, width)
        for a, m in blocks:
            t = lax.dot_general(ev[a : a + m, :], hn, (((1,), (1,)), ((), ())), preferred_element_type=jnp.float32)
            t = t * INV_SCALE
            ids = me * vocab + a + lax.broadcasted_iota(jnp.int32, (m, ROWS), 0)
            t = jnp.where(ids < VOCAB_REAL, t, -jnp.inf)
            zt[a : a + m, :] = t
            top = jnp.maximum(top, jnp.max(t, axis=0, keepdims=True))
        return top

    full_tiles = vocab // 128
    tail = vocab - full_tiles * 128

    def local_lse(n, top):
        lb = label_rows(n)

        def part(a, m, s, t):
            v = zt[pl.ds(a, m), :]
            ids = a + lax.broadcasted_iota(jnp.int32, (m, ROWS), 0)
            e = jnp.exp(v - top).reshape(m // 8, 8, ROWS)
            hit = jnp.where(ids == lb, v, 0.0).reshape(m // 8, 8, ROWS)
            return s + jnp.sum(e, axis=0), t + jnp.sum(hit, axis=0)

        zero = jnp.zeros((8, ROWS), jnp.float32)
        s, t = lax.fori_loop(0, full_tiles, lambda i, v: part(pl.multiple_of(i * 128, 128), 128, *v), (zero, zero), unroll=4)
        s, t = part(full_tiles * 128, tail, s, t)
        tacc[1:2, :] += weights(n) * jnp.sum(t, axis=0, keepdims=True)
        return top + jnp.log(jnp.sum(s, axis=0, keepdims=True))

    def merge(ref, slot, count):
        rows = [ref[slot, q] for q in range(count)]
        top = functools.reduce(jnp.maximum, rows)
        return top + jnp.log(sum(jnp.exp(r - top) for r in rows))

    def grad_logits(k, lse):
        lb = label_rows(k)
        w = weights(k)
        for a, m in [(i * 128, 128) for i in range(full_tiles)] + [(full_tiles * 128, tail)]:
            ids = a + lax.broadcasted_iota(jnp.int32, (m, ROWS), 0)
            p = jnp.exp(zt[a : a + m, :] - lse)
            d = (jnp.where(ids == lb, p - 1.0, p) * w).astype(jnp.bfloat16)
            dzt[a : a + m, :] = d
            dz[:, a : a + m] = d.T

    def embed_grad(k, half):
        tile = width // 4
        for a, m in blocks:
            for j in (2 * half, 2 * half + 1):
                cols = pl.ds(j * tile, tile)
                acc[a : a + m, cols] += jnp.dot(dzt[a : a + m, :], h[k % 3, :, :, cols].reshape(ROWS, tile), preferred_element_type=jnp.float32)

    split = width * 3 // 4
    parts = (pl.ds(0, split), pl.ds(split, width - split))

    def send_p(part):
        cols = parts[part]
        return send(op.at[2, :, :, :, :, cols], r0.at[:, :, :, :, cols], sem_p.at[0, part], sem_p.at[1, part], partner)

    def hidden_grad(k, part):
        own = par(k)
        where = ((1 - c) * own + c * 2, c * own + (1 - c) * 2)
        cols = parts[part]
        r = jnp.dot(dz[...], ev[:, cols], preferred_element_type=jnp.float32)
        for q in range(2):
            op[where[q], :, :, :, :, cols] = r[q * 128 : (q + 1) * 128].reshape(4, 2, 2, 8, cols.size)
        if part == 0:
            @pl.when(k >= 1)
            def _():
                pl.semaphore_wait(cred, 1)
        send_p(part).start()

    def add_partner(k):
        for half in range(2):
            send_p(half).wait()

        def body(i, _):
            op[par(k), i] += r0[i]
            return 0

        lax.fori_loop(0, 4, body, 0)

        @pl.when(k < n_chunks - 1)
        def _():
            pl.semaphore_signal(cred, 1, device_id=partner, device_id_type=MESH)

    def peer(q):
        qy, qx, qc = (q // 4) % 2, (q // 2) % 2, q % 2
        return dev((z + q // 8) % 4, y + qy * (1 - 2 * y), x + qx * (1 - 2 * x), c + qc * (1 - 2 * c))

    def swap8(buf, slot, sem):
        return [send(buf.at[slot, 0], buf.at[slot, q], sem.at[0, slot, q], sem.at[1, slot, q], peer(q)) for q in range(1, 8)]

    def swap32(buf, slot, sem):
        out = []
        for q in range(1, 32):
            there = ((4 - q // 8) % 4) * 8 + q % 8
            out.append(send(buf.at[slot, 0], buf.at[slot, there], sem.at[0, slot, q], sem.at[1, slot, there], peer(q)))
        return out

    def swap4(buf, slot, sem):
        return [
            send(buf.at[slot, 0], buf.at[slot, 4 - q], sem.at[0, slot, q], sem.at[1, slot, 4 - q], peer(8 * q))
            for q in range(1, 4)
        ]

    def start(copies):
        for cp in copies:
            cp.start()

    def wait(copies):
        for cp in copies:
            cp.wait_send()
        for cp in copies:
            cp.wait_recv()

    def z_copies(zr, zl, s1, sl, t, zslot, sem, par):
        ways = []
        for way, (buf, to, block) in enumerate(((zr, nbr_r, 3 - t), (zl, nbr_l, t))):
            sems = (sem.at[0, way, t, par], sem.at[1, way, t, par])
            first = send(s1.at[sl, block], buf.at[t, zslot], *sems, to)
            later = send(buf.at[t - 1, zslot], buf.at[t, zslot], *sems, to) if t else None
            behind, ahead = (z, 3 - z) if way == 0 else (3 - z, z)
            ways.append((behind, ahead, first, later))
        return ways

    def z_wait(ways, t):
        for behind, ahead, first, _ in ways:
            @pl.when((behind <= t) & (ahead > 0))
            def _(first=first):
                first.wait_send()

            @pl.when((behind > 0) & (behind <= t + 1))
            def _(first=first):
                first.wait_recv()

    def z_start(ways, zr, zl, s1, sl, t, zslot):
        for (behind, ahead, first, later), buf, block in zip(ways, (zr, zl), (3 - t + z, t - 3 + z)):
            @pl.when(behind == 0)
            def _(first=first):
                first.start()

            if t:
                @pl.when((behind > 0) & (behind <= t) & (ahead > 0))
                def _(buf=buf, block=block, later=later):
                    buf[t - 1, zslot] += s1[sl, block]
                    later.start()

    def in_range(k):
        return (k >= 0) & (k < n_chunks)

    def two_axes(axis, col, size, r1, zr, zl, fs, fk, r3, sem):
        cols = pl.ds(col, size)
        first_nbr, last_nbr = (nbr_x, nbr_y) if axis == "x" else (nbr_y, nbr_x)
        q = y if axis == "x" else x

        def first(k):
            src = op.at[par(k), :, :, 1 - x, :, cols] if axis == "x" else op.at[par(k), :, 1 - y, :, :, cols]
            return hop(src, r1.at[k % 3], sem["first"], k, first_nbr)

        def last_hop(k):
            return hop(fs, r3.at[par(k)], sem["last"], k, last_nbr)

        def zc(k, t):
            return z_copies(zr, zl, r1, k % 3, t, par(k), sem["z"], par(k))

        def open_up(s):
            @pl.when(in_range(s))
            def _():
                first(s).start()

        def turn(s):
            k = s - 3

            @pl.when(in_range(k))
            def _():
                last_hop(k).wait()
                dhf[:, cols] = fk[...] + r3[par(k)]

            k2 = s - 2

            @pl.when(in_range(k2))
            def _():
                z_wait(zc(k2, 2), 2)
                sl, zs = k2 % 3, par(k2)
                fs[...] = r1[sl, z, 1 - q]
                fk[...] = r1[sl, z, q]
                for cond, buf in ((z >= 1, zr), (z <= 2, zl)):
                    @pl.when(cond)
                    def _(buf=buf):
                        fs[...] += buf[2, zs, 1 - q]
                        fk[...] += buf[2, zs, q]

                last_hop(k2).start()

            k1 = s - 1

            @pl.when(in_range(k1))
            def _():
                first(k1).wait()
                for b in range(4):
                    kept = op[par(k1), b, :, x, :, cols] if axis == "x" else op[par(k1), b, y, :, :, cols]
                    r1[k1 % 3, b] += kept
                z_start(zc(k1, 0), zr, zl, r1, k1 % 3, 0, par(k1))

        def move(s, t):
            k = s - 2

            @pl.when(in_range(k))
            def _():
                z_wait(zc(k, t - 1), t - 1)
                z_start(zc(k, t), zr, zl, r1, k % 3, t, par(k))

        return open_up, turn, move

    def three_axes():
        cols = pl.ds(COL_A + COL_B, COL_C)

        def first(k):
            return hop(op.at[par(k), :, :, 1 - x, :, cols], r1c.at[k % 3], sem_c["first"], k, nbr_x)

        def second(k):
            return hop(r1c.at[k % 3, :, 1 - y], r2c.at[k % 3], sem_c["last"], k, nbr_y)

        def zc(k, t):
            return z_copies(zrc, zlc, r2c, k % 3, t, par(k), sem_c["z"], par(k))

        def open_up(s):
            @pl.when(in_range(s))
            def _():
                first(s).start()

        end = n_chunks - 1

        def to_z(k):
            second(k).wait()
            for b in range(4):
                r2c[k % 3, b] += r1c[k % 3, b, y]
            z_start(zc(k, 0), zrc, zlc, r2c, k % 3, 0, par(k))

        def along_z(k, t):
            z_wait(zc(k, t - 1), t - 1)
            z_start(zc(k, t), zrc, zlc, r2c, k % 3, t, par(k))

        def off_z(k):
            z_wait(zc(k, 2), 2)
            dhf[:, cols] = r2c[k % 3, z]
            for cond, buf in ((z >= 1, zrc), (z <= 2, zlc)):
                @pl.when(cond)
                def _(buf=buf):
                    dhf[:, cols] += buf[2, par(k)]

        def turn(s):
            @pl.when(in_range(s - 3) & (s - 3 != end))
            def _():
                off_z(s - 3)

            @pl.when(in_range(s - 2) & (s - 2 != end))
            def _():
                to_z(s - 2)

            @pl.when(s - 2 == end)
            def _():
                along_z(end, 1)

            k1 = s - 1

            @pl.when(in_range(k1))
            def _():
                first(k1).wait()
                for b in range(4):
                    r1c[k1 % 3, b] += op[par(k1), b, :, x, :, cols]
                second(k1).start()

        def move(s, t):
            @pl.when(in_range(s - 3) & (s - 3 != end))
            def _():
                along_z(s - 3, t)

            if t == 1:
                @pl.when(s - 3 == end)
                def _():
                    along_z(end, 2)
            else:
                @pl.when(s - 2 == end)
                def _():
                    to_z(end)

                @pl.when(s - 3 == end)
                def _():
                    off_z(end)

        return open_up, turn, move

    open_a, turn_a, move_a = two_axes("x", 0, COL_A, r1a, zra, zla, fsa, fka, r3a, sem_a)
    open_b, turn_b, move_b = two_axes("y", COL_A, COL_B, r1b, zrb, zlb, fsb, fkb, r3b, sem_b)
    open_c, turn_c, move_c = three_axes()

    def finish(k, beside=()):
        load_own(k).wait()

        @pl.when(k >= 2)
        def _():
            store_dx(k - 2).wait()

        xo = xr[par(k)].astype(jnp.float32)
        dh = dhf[...] * INV_SCALE
        u = dh * gain[...]
        inv = lax.rsqrt(jnp.mean(xo * xo, axis=-1, keepdims=True) + NORM_EPS)
        slope = inv * jnp.mean(u * xo, axis=-1, keepdims=True)
        xh = xo * inv
        dgacc[...] += dh * xh
        dxb[par(k)] = inv * (u - xh * slope)
        for work in beside:
            work()
        store_dx(k).start()

    def tell_neighbours():
        pl.semaphore_signal(nbr.at[0], 1, device_id=nbr_x, device_id_type=MESH)
        pl.semaphore_signal(nbr.at[1], 1, device_id=nbr_y, device_id_type=MESH)

        @pl.when(z <= 2)
        def _():
            pl.semaphore_signal(nbr.at[2], 1, device_id=nbr_r, device_id_type=MESH)

        @pl.when(z >= 1)
        def _():
            pl.semaphore_signal(nbr.at[3], 1, device_id=nbr_l, device_id_type=MESH)

    def hear_neighbours():
        pl.semaphore_wait(nbr.at[0], 1)
        pl.semaphore_wait(nbr.at[1], 1)

        @pl.when(z >= 1)
        def _():
            pl.semaphore_wait(nbr.at[2], 1)

        @pl.when(z <= 2)
        def _():
            pl.semaphore_wait(nbr.at[3], 1)

    with jax.named_scope("init"):
        for half in range(2):
            load_x(0, half).start()
        for j in range(len(blocks)):
            tab_block(j).start()
        barrier = pltpu.get_barrier_semaphore()
        for q in range(1, 32):
            pl.semaphore_signal(barrier, 1, device_id=peer(q), device_id_type=MESH)
        tacc[...] = jnp.zeros_like(tacc)
        tacc[2:3, :] = jnp.broadcast_to(jnp.sum(tok[1], keepdims=True), (1, ROWS))
        dgacc[...] = jnp.zeros_like(dgacc)
    with jax.named_scope("norm0"):
        for half in range(2):
            load_x(0, half).wait()
        norm(0)
        for half in range(2):
            load_x(1, half).start()
        for j in range(len(blocks)):
            tab_block(j).wait()

    last = n_chunks + DEPTH

    def iteration(i, _):
        s = i - 1
        busy = in_range(s)
        ahead = i < n_chunks
        scope = jax.named_scope

        with scope("logits"):
            @pl.when(ahead)
            def _():
                top = logits(i)
                st[par(i), 0] = local_lse(i, top)

        with scope("tell"):
            @pl.when(i == 0)
            def _():
                pl.semaphore_wait(barrier, 31)

            @pl.when(ahead)
            def _():
                start(swap32(st, par(i), sem_st))

        with scope("b0"):
            turn_b(s)

        with scope("partner"):
            @pl.when(busy)
            def _():
                add_partner(s)

            open_a(s)
            open_b(s)
            open_c(s)

        with scope("zero"):
            @pl.when(i == 0)
            def _():
                acc[...] = jnp.zeros_like(acc)

        with scope("de0"):
            @pl.when(busy)
            def _():
                embed_grad(s, 0)

        with scope("ac0"):
            turn_a(s)
            turn_c(s)

            @pl.when((i >= 1) & (i < last - 1))
            def _():
                tell_neighbours()

        with scope("finish"):
            @pl.when(busy & (s >= 3))
            def _():
                finish(s - 3, (lambda: embed_grad(s, 1),))

            @pl.when(busy & (s < 3))
            def _():
                embed_grad(s, 1)

            @pl.when(s >= n_chunks)
            def _():
                finish(s - 3)

            @pl.when(in_range(s - 2))
            def _():
                load_own(s - 2).start()

        with scope("de1"):
            @pl.when(i == n_chunks)
            def _():
                pltpu.make_async_copy(acc, de_out, sem_out.at[2]).start()

        with scope("hear"):
            @pl.when((i >= 1) & (i < last - 1))
            def _():
                hear_neighbours()

        with scope("b1"):
            move_b(i, 1)

        with scope("norm"):
            @pl.when(i + 1 < n_chunks)
            def _():
                for half in range(2):
                    load_x(i + 1, half).wait()
                norm(i + 1)

            @pl.when(i + 2 < n_chunks)
            def _():
                for half in range(2):
                    load_x(i + 2, half).start()

        with scope("stat"):
            @pl.when(ahead)
            def _():
                wait(swap32(st, par(i), sem_st))

        with scope("dz"):
            @pl.when(ahead)
            def _():
                lse = merge(st, par(i), 32)
                tacc[0:1, :] += weights(i) * lse
                grad_logits(i, lse)

        with scope("ac1"):
            move_a(i, 1)
            move_c(i, 1)

        with scope("dh0"):
            @pl.when(ahead)
            def _():
                hidden_grad(i, 0)

        with scope("b2"):
            move_b(i, 2)

        with scope("dh1"):
            @pl.when(ahead)
            def _():
                hidden_grad(i, 1)

        with scope("ac2"):
            move_a(i, 2)
            move_c(i, 2)

        return 0

    lax.fori_loop(0, last + 1, iteration, 0)
    with jax.named_scope("gain"):
        dg1[0, 0, :, 0:width] = jnp.sum(dgacc[...], axis=0, keepdims=True)
        dg1[0, 0, :, width : width + ROWS] = tacc[1:2, :]
        start(swap8(dg1, 0, sem_g1))
        wait(swap8(dg1, 0, sem_g1))
        dg2[0, 0] = sum(dg1[0, q] for q in range(8))
        start(swap4(dg2, 0, sem_g2))
        wait(swap4(dg2, 0, sem_g2))
        total = sum(dg2[0, q] for q in range(4))
        sums_out[:, 0:width] = total[:, 0:width]
        sums_out[:, width : width + ROWS] = tacc[0:1, :] - total[:, width : width + ROWS]
        for n in (n_chunks - 2, n_chunks - 1):
            store_dx(n).wait()
        pltpu.make_async_copy(acc, de_out, sem_out.at[2]).wait()


def hand_over_kernel(de_in, dx_in, sums_in, de_out, dx_out, dg_out, loss_out, buf, row, sem, row_sem):
    step = buf.shape[1]
    gets, puts = [], []
    for src, dst in ((de_in, de_out), (dx_in, dx_out)):
        rows = src.shape[0]
        for r in range(0, rows, step):
            n, some = len(gets), pl.ds(r, min(step, rows - r))
            here = buf.at[n, pl.ds(0, some.size)]
            gets.append(pltpu.make_async_copy(src.at[some], here, sem.at[0, n]))
            puts.append(pltpu.make_async_copy(here, dst.at[some], sem.at[1, n]))
    for get in gets:
        get.start()
    width = de_in.shape[1]
    get_row = pltpu.make_async_copy(sums_in, row, row_sem.at[0])
    put_row = pltpu.make_async_copy(row.at[:, pl.ds(0, width)], dg_out, row_sem.at[1])
    get_row.start()
    get_row.wait()
    put_row.start()
    loss_out[...] = jnp.sum(row[:, width : width + ROWS], keepdims=True)
    for get in gets:
        get.wait()
    scaled = de_in.shape[0]
    for n, put in enumerate(puts):
        if n * step < scaled:
            buf[n] = buf[n] * INV_SCALE
        put.start()
    for put in (put_row, *puts):
        put.wait()


def solution(mesh):
    def local_step(residual, labels, loss_mask, norm_gain, table_shard):
        tokens, width = residual.shape
        vocab = table_shard.shape[0]
        n_chunks = tokens // ROWS
        f32, bf16 = jnp.float32, jnp.bfloat16

        tok = jnp.stack([labels.astype(f32), loss_mask]).reshape(2, 16, 2, n_chunks, GROUP)
        tok = tok.transpose(0, 3, 2, 1, 4).reshape(2, n_chunks, ROWS)
        dma = pltpu.SemaphoreType.DMA
        vm = pltpu.VMEM
        slab = (GROUP, width)
        pair, ways = (2, 2), (2, 2, 3, 2)
        scratch = [vm((vocab, width), bf16), vm((3, 32, *slab), bf16), vm((vocab, ROWS), f32)]
        scratch += [vm((vocab, ROWS), bf16), vm((ROWS, vocab), bf16), vm((vocab, width), f32)]
        scratch += [vm((3, *GRID, *slab), f32), vm((*GRID, *slab), f32)]
        scratch += [vm((3, 4, 2, GROUP, n), f32) for n in (COL_A, COL_B)]
        scratch += [vm((3, 4, 2, GROUP, COL_C), f32), vm((3, 4, GROUP, COL_C), f32)]
        for n in (COL_A, COL_B):
            scratch += [vm((3, 2, 2, GROUP, n), f32)] * 2
        scratch += [vm((3, 2, GROUP, COL_C), f32)] * 2
        for n in (COL_A, COL_B):
            scratch += [vm((GROUP, n), f32), vm((GROUP, n), f32), vm((2, GROUP, n), f32)]
        scratch += [vm((2, 32, 1, ROWS), f32), vm((GROUP, ROWS), f32), vm((32, GROUP, 128), f32)]
        scratch += [vm(slab, f32), vm((2, *slab), bf16), vm((2, *slab), f32), vm(slab, f32)]
        scratch += [vm((1, n, 1, width + ROWS), f32) for n in (8, 4)]
        scratch += [dma((4,)), dma((8,)), dma((3,)), dma(pair), pltpu.SemaphoreType.REGULAR, pltpu.SemaphoreType.REGULAR((4,))]
        scratch += [dma((2, 2, 32)), dma((2, 1, 8)), dma((2, 1, 4))]
        scratch += [{"first": dma(pair), "z": dma(ways), "last": dma(pair)} for _ in "abc"]
        whole = pl.BlockSpec(memory_space=pltpu.VMEM)
        raw = pl.BlockSpec(memory_space=pl.ANY)
        dx, de, sums = pl.pallas_call(
            functools.partial(step_kernel, n_chunks),
            out_shape=(
                jax.ShapeDtypeStruct((n_chunks, GROUP, width), f32),
                jax.ShapeDtypeStruct((vocab, width), f32),
                jax.ShapeDtypeStruct((1, width + ROWS), f32),
            ),
            in_specs=[raw, whole, whole, raw],
            out_specs=(raw, raw, whole),
            scratch_shapes=scratch,
            compiler_params=pltpu.CompilerParams(vmem_limit_bytes=VMEM_LIMIT, has_side_effects=True, collective_id=0),
            name="head_step",
        )(
            residual.reshape(16, 2, n_chunks, GROUP, width),
            tok,
            norm_gain.reshape(1, width),
            table_shard,
        )
        de, dx, dg, loss = pl.pallas_call(
            hand_over_kernel,
            out_shape=(
                jax.ShapeDtypeStruct((vocab, width), f32),
                jax.ShapeDtypeStruct((n_chunks * GROUP, width), f32),
                jax.ShapeDtypeStruct((1, width), f32),
                jax.ShapeDtypeStruct((1, 1), f32),
            ),
            in_specs=[raw] * 3,
            out_specs=(raw, raw, raw, whole),
            scratch_shapes=[vm((16, 128, width), f32), vm((1, width + ROWS), f32), dma((2, 16)), dma((2,))],
            compiler_params=pltpu.CompilerParams(vmem_limit_bytes=VMEM_LIMIT),
            name="hand_over",
        )(de, dx.reshape(n_chunks * GROUP, width), sums)
        return loss.reshape(()), dx, de, dg.reshape(width)

    return jax.shard_map(local_step, mesh=mesh, in_specs=(P(), P(), P(), P(), P("vp", None)), out_specs=(P(), P("vp", None), P("vp", None), P()), check_vma=False)
```
